32 devices in a mesh: groups: 2 (over x), patch: 16 (over z, y, core).
Axes of the slice: x: 2, y: 2, z: 4, core: 2. Of those that a mesh axis runs over, the one named last changes fastest.
Arguments:
- queries: bfloat16 [1024, 1536], P(('groups', 'patch')), parts along dimension 0, may hold values from -8 to 8
- fresh_keys: bfloat16 [1024, 1536], P(('groups', 'patch')), parts along dimension 0, may hold values from -8 to 8
- fresh_values: bfloat16 [1024, 1536], P(('groups', 'patch')), parts along dimension 0, may hold values from -128 to 128
- stale_keys: bfloat16 [1024, 1536], P(('groups', 'patch')), parts along dimension 0, may hold values from -8 to 8
- stale_values: bfloat16 [1024, 1536], P(('groups', 'patch')), parts along dimension 0, may hold values from -128 to 128
- text_keys: bfloat16 [452, 1536], P('groups'), parts along dimension 0, may hold values from -8 to 8
- text_values: bfloat16 [452, 1536], P('groups'), parts along dimension 0, may hold values from -128 to 128
- out_weight: bfloat16 [1536, 3072], P(None, 'patch'), may hold values from -0.15625 to 0.15625
- gate_table: float32 [50, 3072], replicated, may hold values from 0.1 to 1.9
- timestep: int32 [2], P('groups'), parts along dimension 0, may hold values from 0 to 49
Outputs:
- branch: bfloat16 [1024, 3072], P(('groups', 'patch')), parts along dimension 0
The draws below stay inside these ranges and needn't reach their ends.
There are 2 independent parts, one for each index of `groups`. The reference program is written for one: setup_inputs(seed, part) draws one part's arguments, and reference() takes and returns one part's arrays. A program takes and returns all parts, laid end to end along the dimension named above; an argument that names none is the same for every part. Nothing has to cross between parts.
All inputs are finite; a program needn't handle non-finite values.
Results may differ from the reference program's by a relative error of at most 0.0095.
Values may be sent and summed in bfloat16 or wider, within the bound.
A program may use at most 128 MiB of HBM per device.

```python
import jax
import jax.numpy as jnp
from jax import lax

D = 3072
HEAD_DIM = 64
TEXT = 226
HEADS = 24
STEPS = 50
TOK_DEV = 32
TOKENS = 512
N_PATCH = 16


def draw_queries(key, part):
    normal_part = jax.random.truncated_normal(jax.random.fold_in(key, 1), -8.0, 8.0, (TOKENS, HEADS * HEAD_DIM), jnp.float32)
    return normal_part.astype(jnp.bfloat16)


def draw_text_keys(key, part):
    normal_part = jax.random.truncated_normal(jax.random.fold_in(key, 2), -8.0, 8.0, (TEXT, HEADS * HEAD_DIM), jnp.float32)
    return normal_part.astype(jnp.bfloat16)


def shard_levels(stream_key, dims, split, least, largest):
    factor_of = 1.0
    for position, blocks in split:
        steps = jax.random.uniform(jax.random.fold_in(jax.random.fold_in(stream_key, 6), position), (blocks,), jnp.float32, least / len(split), largest / len(split))
        factor_of = factor_of * jnp.repeat(jnp.exp(steps), dims[position] // blocks).reshape((-1,) + (1,) * (len(dims) - 1 - position))
    return factor_of


def scatter_about(own_key, extent, deviation, reach, shards=(), kind=jnp.bfloat16):
    values = deviation * jax.random.normal(own_key, extent, jnp.float32)
    if shards:
        values = values * shard_levels(own_key, extent, shards, -0.22, 0.18)
    return jnp.clip(values, -reach, reach).astype(kind)


def setup_inputs(seed: int = 0, part: int = 0) -> dict:
    splits = jax.random.split(jax.random.key(seed), 11)
    part_splits = jax.random.split(jax.random.fold_in(splits[10], part), 11)
    return {
        "queries": draw_queries(jax.random.fold_in(jax.random.fold_in(splits[10], part), 71), part),
        "fresh_keys": scatter_about(part_splits[1], (TOKENS, HEADS * HEAD_DIM), 1.0, 8.0, ((0, 16),)),
        "fresh_values": scatter_about(part_splits[2], (TOKENS, HEADS * HEAD_DIM), 24.0, 128.0, ((0, 16),)),
        "stale_keys": scatter_about(part_splits[3], (TOKENS, HEADS * HEAD_DIM), 1.0, 8.0, ((0, 16),)),
        "stale_values": scatter_about(part_splits[4], (TOKENS, HEADS * HEAD_DIM), 24.0, 128.0, ((0, 16),)),
        "text_keys": draw_text_keys(jax.random.fold_in(jax.random.fold_in(splits[10], part), 71), part),
        "text_values": scatter_about(part_splits[6], (TEXT, HEADS * HEAD_DIM), 24.0, 128.0),
        "out_weight": scatter_about(splits[7], (HEADS * HEAD_DIM, D), (HEADS * HEAD_DIM) ** -0.5, 0.15625, ((1, 16),)),
        "gate_table": jnp.clip(1.0 + 0.18 * jax.random.normal(splits[8], (STEPS, D), jnp.float32), 0.1, 1.9),
        "timestep": jax.random.randint(part_splits[9], (1,), 0, STEPS).astype(jnp.int32),
    }


def reference(queries, fresh_keys, fresh_values, stale_keys, stale_values, text_keys, text_values, out_weight, gate_table, timestep):
    gating = gate_table[timestep[0]]
    scaling = HEAD_DIM ** -0.5

    def one_patch(patch_id):
        offset = (patch_id * TOK_DEV).astype(jnp.int32)
        query = lax.dynamic_slice_in_dim(queries, offset, TOK_DEV, 0).astype(jnp.float32).reshape(TOK_DEV, HEADS, HEAD_DIM)
        key_video = lax.dynamic_update_slice_in_dim(stale_keys, lax.dynamic_slice_in_dim(fresh_keys, offset, TOK_DEV, 0), offset, 0)
        value_video = lax.dynamic_update_slice_in_dim(stale_values, lax.dynamic_slice_in_dim(fresh_values, offset, TOK_DEV, 0), offset, 0)
        key_rows = jnp.concatenate([text_keys, key_video], 0).astype(jnp.float32).reshape(-1, HEADS, HEAD_DIM)
        value_rows = jnp.concatenate([text_values, value_video], 0).astype(jnp.float32).reshape(-1, HEADS, HEAD_DIM)
        scores = jnp.einsum("thd,shd->ths", query, key_rows) * scaling
        highest = jnp.max(scores, -1)
        expo = jnp.exp(scores - highest[..., None])
        total = jnp.sum(expo, -1)
        probs = lax.optimization_barrier(expo.astype(jnp.bfloat16)).astype(jnp.float32)
        weighted = jnp.einsum("ths,shd->thd", probs, value_rows)
        attended = (weighted / total[..., None]).reshape(TOK_DEV, HEADS * HEAD_DIM).astype(jnp.bfloat16)
        projected = jnp.dot(attended, out_weight, preferred_element_type=jnp.float32)
        return (projected * gating[None, :]).astype(jnp.bfloat16)

    blocks = lax.map(one_patch, jnp.arange(N_PATCH, dtype=jnp.int32))
    return blocks.reshape(TOKENS, D)
```

```python
import functools
import math

import jax
import jax.numpy as jnp
from jax import lax
from jax.experimental import pallas as pl
from jax.experimental.pallas import tpu as pltpu
from jax.sharding import PartitionSpec as P

HEAD_DIM = 64
HEADS = 24


def from_behind(shard, axis, by):
    peers = lax.axis_size(axis)
    return lax.ppermute(shard, axis, [(i, (i + by) % peers) for i in range(peers)])


def pick_group(stacked, position):
    return lax.dynamic_index_in_dim(stacked, position, 0, keepdims=False)


def by_group(matrix, group_count):
    width = matrix.shape[1] // group_count
    return matrix.reshape(matrix.shape[0], group_count, width).transpose(1, 0, 2)


def gather_block(stacked, group_count, position):
    received = [pick_group(stacked, position)]
    for step_size in range(1, group_count):
        payload = pick_group(stacked, (position + step_size) % group_count)
        arrived = []
        for offset_by in (step_size, step_size - group_count):
            arrived.append(from_behind(payload, "patch", offset_by))
        received.append(jnp.where(position >= step_size, arrived[0], arrived[1]))
    ordered = jnp.stack(received, 0)
    order = (position - jnp.arange(group_count, dtype=jnp.int32)) % group_count
    return jnp.take(ordered, order, axis=0)


def return_block(stacked, group_count, position):
    received = [pick_group(stacked, position)]
    for step_size in range(1, group_count):
        payload = pick_group(stacked, (position + step_size) % group_count)
        arrived = []
        for offset_by in (step_size, step_size - group_count):
            arrived.append(from_behind(payload, "patch", offset_by))
        received.append(jnp.where(position >= step_size, arrived[0], arrived[1]))
    ordered = jnp.stack(received, 0)
    order = (position - jnp.arange(group_count, dtype=jnp.int32)) % group_count
    return jnp.take(ordered, order, axis=0)


def body(
    queries,
    fresh_keys,
    fresh_values,
    stale_keys,
    stale_values,
    text_keys,
    text_values,
    out_weight,
    gate_table,
    timestep,
):
    row_count = queries.shape[0]
    head_count = HEADS
    head_width = HEAD_DIM
    scaling = head_width ** (-0.5)
    group_count = math.gcd(head_count, 8)
    group_heads = head_count // group_count
    group_width = group_heads * head_width
    device_count = lax.axis_size("patch")
    position = lax.axis_index("patch") % group_count
    block_first = lax.axis_index("patch") // group_count * group_count
    local_stack = jnp.stack(
        [
            by_group(queries, group_count),
            by_group(fresh_keys, group_count),
            by_group(fresh_values, group_count),
        ],
        1,
    )
    block_stack = gather_block(local_stack, group_count, position)
    block_rows_count = group_count * row_count
    block_query = block_stack[:, 0].reshape(block_rows_count, group_heads, head_width)
    block_keys = block_stack[:, 1].reshape(block_rows_count, group_heads, head_width)
    block_values = block_stack[:, 2].reshape(block_rows_count, group_heads, head_width)
    spread_keys = jnp.tile(by_group(stale_keys, group_count), (device_count // group_count, 1, 1))
    spread_values = jnp.tile(
        by_group(stale_values, group_count), (device_count // group_count, 1, 1)
    )
    every_keys, every_values = (
        lax.all_to_all(spread_keys, "patch", split_axis=0, concat_axis=0, tiled=True),
        lax.all_to_all(spread_values, "patch", split_axis=0, concat_axis=0, tiled=True),
    )
    every_keys = every_keys.reshape(device_count * row_count, group_heads, head_width)
    every_values = every_values.reshape(device_count * row_count, group_heads, head_width)
    text_k = pick_group(by_group(text_keys, group_count), position).reshape(
        -1, group_heads, head_width
    )
    text_v = pick_group(by_group(text_values, group_count), position).reshape(
        -1, group_heads, head_width
    )
    query_patch = jnp.arange(block_rows_count, dtype=jnp.int32) // row_count
    stale_patch = jnp.arange(device_count * row_count, dtype=jnp.int32) // row_count
    stale_mask = stale_patch[None, :] != (block_first + query_patch)[:, None]
    fresh_mask = query_patch[None, :] == query_patch[:, None]

    def scored(key_block):
        return (
            jnp.einsum("qhd,khd->qhk", block_query, key_block, preferred_element_type=jnp.float32)
            * scaling
        )

    text_scores = scored(text_k)
    fresh_scores = jnp.where(fresh_mask[:, None, :], scored(block_keys), -1e30)
    stale_scores = jnp.where(stale_mask[:, None, :], scored(every_keys), -1e30)
    highest = jnp.maximum(
        jnp.maximum(jnp.max(text_scores, -1), jnp.max(fresh_scores, -1)), jnp.max(stale_scores, -1)
    )
    text_expo = jnp.exp(text_scores - highest[..., None])
    fresh_expo = jnp.exp(fresh_scores - highest[..., None])
    stale_expo = jnp.exp(stale_scores - highest[..., None])
    total = jnp.sum(text_expo, -1) + jnp.sum(fresh_expo, -1) + jnp.sum(stale_expo, -1)

    def weigh_block(expo, value_block):
        return jnp.einsum(
            "qhk,khd->qhd",
            expo.astype(jnp.bfloat16),
            value_block,
            preferred_element_type=jnp.float32,
        )

    weighted = (
        weigh_block(text_expo, text_v)
        + weigh_block(fresh_expo, block_values)
        + weigh_block(stale_expo, every_values)
    )
    block_out = (
        (weighted / total[..., None])
        .reshape(group_count, row_count, group_width)
        .astype(jnp.bfloat16)
    )
    home = return_block(block_out, group_count, position)
    attended = home.transpose(1, 0, 2).reshape(row_count, head_count * head_width)
    projected = jnp.dot(
        attended,
        lax.all_gather(out_weight, "patch", axis=1, tiled=True),
        preferred_element_type=jnp.float32,
    )
    selector = (jnp.arange(gate_table.shape[0], dtype=jnp.int32) == timestep[0]).astype(jnp.float32)
    gating = jnp.dot(selector, gate_table, precision=lax.Precision.HIGHEST)
    return (projected * gating[None, :]).astype(jnp.bfloat16)


LANES = 128
CORES = 2
HALVES = 2
PARTS = 4
NEVER = -1e30
MESH = pl.DeviceIdType.MESH


def fused_fits(mesh):
    chips = mesh.shape["patch"] // CORES
    return (
        2 * HEAD_DIM == LANES
        and mesh.shape["patch"] % (2 * CORES) == 0
        and HEADS == 3 * chips
        and chips == math.gcd(HEADS, 8)
        and chips == 4 * CORES
    )


def swap_halves(tile):
    return pltpu.roll(tile.astype(jnp.float32), HEAD_DIM, 1).astype(tile.dtype)


def low_lanes(rows):
    return lax.broadcasted_iota(jnp.int32, (rows, LANES), 1) < HEAD_DIM


def odd_pair(first, second, upper):
    low = low_lanes(first.shape[0])
    if upper:
        return jnp.where(low, swap_halves(first), second)
    return jnp.where(low, first, swap_halves(second))


def score(query, keys):
    return lax.dot_general(query, keys, (((1,), (1,)), ((), ())), preferred_element_type=jnp.float32)


def weigh(probs, values):
    return jnp.dot(probs, values, preferred_element_type=jnp.float32)


def fused_kernel(
    devices,
    q_ref,
    kf_ref,
    vf_ref,
    ks_ref,
    vs_ref,
    tk_ref,
    tv_ref,
    w_ref,
    g_ref,
    t_ref,
    out_ref,
    rows_in,
    text_in,
    gate_in,
    weights,
    weight,
    send_fresh,
    send_stale,
    fresh,
    stale,
    text,
    piece,
    pieces,
    product,
    load_sem,
    fresh_send,
    fresh_recv,
    stale_send,
    stale_recv,
    weight_send,
    weight_recv,
    piece_send,
    piece_across,
    piece_forward,
    piece_far,
    piece_recv,
    back_send,
    back_recv,
):
    groups = lax.axis_index("groups")
    me = lax.axis_index("patch")
    chips = devices // CORES
    group_count = chips
    rows = q_ref.shape[0]
    block_rows = group_count * rows
    text_rows = tk_ref.shape[0]
    part_columns = w_ref.shape[0]
    columns = CORES * part_columns
    chip, core = me // CORES, me % CORES
    block, position = me // group_count, me % group_count
    partner = me + 1 - 2 * core
    side, place = chip % 2, chip // 2
    places = chips // 2
    odd_tile = group_count + position // 2

    def device(index):
        return (groups, index)

    def remote(src, dst, send, recv, index):
        return pltpu.make_async_remote_copy(
            src_ref=src,
            dst_ref=dst,
            send_sem=send,
            recv_sem=recv,
            device_id=device(index),
            device_id_type=MESH,
        )

    def weight_rows(of_core):
        start = pl.multiple_of(of_core * part_columns, part_columns)
        return weights.at[pl.ds(start, part_columns), :]

    barrier = pltpu.get_barrier_semaphore()

    @pl.loop(1, devices)
    def _(step):
        pl.semaphore_signal(
            barrier, inc=1, device_id=device((me + step) % devices), device_id_type=MESH
        )

    loads = [
        pltpu.make_async_copy(ref, rows_in.at[i], load_sem.at[i])
        for i, ref in enumerate((q_ref, kf_ref, vf_ref, ks_ref, vs_ref))
    ]
    full_lanes = pl.ds(pl.multiple_of(position * LANES, LANES), LANES)
    odd_lanes = pl.ds(pl.multiple_of(odd_tile * LANES, LANES), LANES)
    for i, (ref, lanes) in enumerate(
        ((tk_ref, full_lanes), (tv_ref, full_lanes), (tk_ref, odd_lanes), (tv_ref, odd_lanes))
    ):
        loads.append(pltpu.make_async_copy(ref.at[:, lanes], text_in.at[i], load_sem.at[5 + i]))
    chip_columns = pl.ds(pl.multiple_of(chip * columns, LANES), columns)
    loads.append(pltpu.make_async_copy(g_ref.at[:, chip_columns], gate_in, load_sem.at[9]))
    loads.append(pltpu.make_async_copy(w_ref, weight_rows(core), load_sem.at[10]))
    for load in loads:
        load.start()

    for load in loads[:5]:
        load.wait()
    for g in range(group_count):
        own = slice(g * LANES, (g + 1) * LANES)
        tile = group_count + g // 2
        odd = slice(tile * LANES, (tile + 1) * LANES)
        upper = g % 2 == 1
        send_fresh[g, 0] = rows_in[0, :, own]
        odd_query = rows_in[0, :, odd]
        odd_query = swap_halves(odd_query) if upper else odd_query
        send_fresh[g, 1] = jnp.where(low_lanes(rows), odd_query, jnp.zeros_like(odd_query))
        send_fresh[g, 2] = rows_in[1, :, own]
        send_fresh[g, 3] = rows_in[2, :, own]
        send_fresh[g, 4] = odd_pair(rows_in[1, :, odd], rows_in[2, :, odd], upper)
        send_stale[g, 0] = rows_in[3, :, own]
        send_stale[g, 1] = rows_in[4, :, own]
        send_stale[g, 2] = odd_pair(rows_in[3, :, odd], rows_in[4, :, odd], upper)

    def patch_rows(index):
        return pl.ds(pl.multiple_of(index * rows, rows), rows)

    def fresh_copy(target, source):
        return remote(
            send_fresh.at[target],
            fresh.at[:, patch_rows(source), :],
            fresh_send.at[target],
            fresh_recv.at[source],
            block * group_count + target,
        )

    def stale_copy(target, source):
        other = (target // group_count + source // group_count) % 2
        return remote(
            send_stale.at[target % group_count],
            stale.at[other, :, patch_rows(source % group_count), :],
            stale_send.at[target],
            stale_recv.at[source],
            target,
        )

    pl.semaphore_wait(barrier, devices - 1)

    @pl.loop(1, group_count)
    def _(step):
        fresh_copy((position + step) % group_count, position).start()

    @pl.loop(1, group_count)
    def _(step):
        stale_copy(block * group_count + (position + step) % group_count, me).start()

    @pl.loop(0, group_count)
    def _(step):
        stale_copy((1 - block) * group_count + (position + step) % group_count, me).start()

    own_copies = (
        pltpu.make_async_copy(
            send_fresh.at[position],
            fresh.at[:, patch_rows(position), :],
            fresh_recv.at[position],
        ),
        pltpu.make_async_copy(
            send_stale.at[position],
            stale.at[0, :, patch_rows(position), :],
            stale_recv.at[me],
        ),
    )
    for copy in own_copies:
        copy.start()
    weight_copy = remote(w_ref, weight_rows(core), weight_send, weight_recv, partner)
    weight_copy.start()

    for load in loads[5:9]:
        load.wait()
    text[...] = jnp.zeros_like(text)
    text[0, :text_rows] = text_in[0]
    text[1, :text_rows] = text_in[1]
    text[2, :text_rows] = jnp.where(
        position % 2 == 1,
        odd_pair(text_in[2], text_in[3], True),
        odd_pair(text_in[2], text_in[3], False),
    )
    loads[9].wait()
    loads[10].wait()
    remote(w_ref, weight_rows(1 - core), weight_send, weight_recv, partner).wait_recv()
    depth = w_ref.shape[1]
    chunk = 2 * LANES

    @pl.loop(0, depth // chunk)
    def _(step):
        at = pl.ds(pl.multiple_of(step * chunk, chunk), chunk)
        weight[at, :] = weights[:, at].T

    scaling = HEAD_DIM**-0.5
    half = block_rows // HALVES
    part_rows = block_rows // PARTS
    odd_rows = part_rows // 2
    padded = text.shape[1]

    def same_patch(stacked, part, keys, first_key):
        query = lax.broadcasted_iota(jnp.int32, (stacked * half, keys), 0) % half + part * half
        key = lax.broadcasted_iota(jnp.int32, (stacked * half, keys), 1) + first_key
        return query // rows == key // rows

    def take(state, scores, values):
        highest, total, weighted = state
        peak = highest
        for each in scores:
            top = jnp.max(each, -1, keepdims=True)
            peak = top if peak is None else jnp.maximum(peak, top)
        sums = sums_of = None
        for each, value in zip(scores, values):
            expo = jnp.exp(each - peak)
            row_sum = jnp.sum(expo, -1, keepdims=True)
            product_of = weigh(expo.astype(jnp.bfloat16), value)
            sums = row_sum if sums is None else sums + row_sum
            sums_of = product_of if sums_of is None else sums_of + product_of
        if highest is None:
            return peak, sums, sums_of
        fade = jnp.exp(highest - peak)
        return peak, total * fade + sums, weighted * fade + sums_of

    @pl.loop(0, group_count)
    def _(source):
        fresh_copy(position, source).wait_recv()

    low = low_lanes(half)
    units = []
    for part in range(HALVES):
        at = slice(part * half, (part + 1) * half)
        pair_query = fresh[0, at] * jnp.asarray(scaling, fresh.dtype)
        nothing = jnp.zeros_like(pair_query)
        both = jnp.concatenate(
            [jnp.where(low, pair_query, nothing), jnp.where(low, nothing, pair_query)], 0
        )
        odd_query = fresh[1, at] * jnp.asarray(scaling, fresh.dtype)
        units.append((part, 2, 0, 1, both))
        units.append((part, 1, 2, 2, odd_query))

    states = []
    for part, stacked, kind, value_kind, query in units:
        at = slice(part * half, (part + 1) * half)
        absent = lax.broadcasted_iota(jnp.int32, (stacked * half, padded), 1) >= text_rows
        text_score = jnp.where(absent, NEVER, score(query, text[kind]))
        fresh_score = jnp.where(
            same_patch(stacked, part, half, part * half),
            score(query, fresh[kind + 2, at]),
            NEVER,
        )
        states.append(
            take(
                (None, None, None),
                (text_score, fresh_score),
                (text[value_kind], fresh[value_kind + 2, at]),
            )
        )

    @pl.loop(0, group_count)
    def _(source):
        stale_copy(me, block * group_count + source).wait_recv()

    for i, (part, stacked, kind, value_kind, query) in enumerate(units):
        own_score = jnp.where(
            same_patch(stacked, part, block_rows, 0), NEVER, score(query, stale[0, kind])
        )
        states[i] = take(states[i], (own_score,), (stale[0, value_kind],))

    @pl.loop(0, group_count)
    def _(source):
        stale_copy(me, (1 - block) * group_count + source).wait_recv()

    def column_copy(part, target_place, source):
        return remote(
            piece.at[part],
            pieces.at[part, source],
            piece_send.at[part, target_place],
            piece_recv.at[part, source],
            (target_place * 2 + side) * CORES + block,
        )

    def across_copy(part):
        return remote(
            piece.at[part],
            pieces.at[part, position],
            piece_across.at[part],
            piece_recv.at[part, position],
            (place * 2 + 1 - side) * CORES + block,
        )

    def forward_copy(part, source, index):
        return remote(
            pieces.at[part, source],
            pieces.at[part, source],
            piece_forward.at[part, index],
            piece_recv.at[part, source],
            (place * 2 + 1 - side) * CORES + core,
        )

    def far_copy(part, source, index):
        return remote(
            pieces.at[part, source],
            pieces.at[part, source],
            piece_far.at[part, index],
            piece_recv.at[part, source],
            ((1 - core) * (places - 1) * 2 + side) * CORES + core,
        )

    mate = 2 * block + 1 - place % 2
    gate = 2 - block
    at_gate = place == 2 - core
    elsewhere = place // 2 != core

    part_low = low_lanes(part_rows)
    odd_low = low_lanes(odd_rows)
    done = []
    for part in range(PARTS):
        if part % (PARTS // HALVES) == 0:
            done = []
            first_unit = 2 * (part * HALVES // PARTS)
            for i in (first_unit, first_unit + 1):
                _, _, kind, value_kind, query = units[i]
                _, total, weighted = take(
                    states[i], (score(query, stale[1, kind]),), (stale[1, value_kind],)
                )
                done.append(weighted / total)
        at = part % (PARTS // HALVES) * part_rows
        piece[part, :part_rows] = jnp.where(
            part_low, done[0][at : at + part_rows], done[0][half + at : half + at + part_rows]
        ).astype(piece.dtype)
        piece[part, part_rows:] = jnp.where(
            odd_low,
            pltpu.roll(done[1][at : at + odd_rows], HEAD_DIM, 1),
            done[1][at + odd_rows : at + part_rows],
        ).astype(piece.dtype)

        column_copy(part, gate, position).start()
        across_copy(part).start()
        column_copy(part, mate, position).start()

        @pl.when(core == block)
        def _():
            pltpu.make_async_copy(
                piece.at[part], pieces.at[part, position], piece_recv.at[part, position]
            ).start()

        @pl.when(core != block)
        def _():
            column_copy(part, place, position).start()

    def column_source(index, of_side):
        return index // CORES * 2 * CORES + of_side * CORES + index % CORES

    column_pieces = group_count // 2

    for part in range(PARTS):

        @pl.loop(0, column_pieces)
        def _(index):
            index = (index + (1 - core) * CORES) % column_pieces
            source = column_source(index, side)
            column_copy(part, place, source).wait_recv()

            @pl.when(at_gate)
            def _():
                far_copy(part, source, index).start()

            @pl.when(elsewhere | (index // CORES != place % 2))
            def _():
                forward_copy(part, source, index).start()

    def back_copy(target, source):
        return remote(
            product.at[target],
            out_ref.at[:, pl.ds(pl.multiple_of(source * columns, LANES), columns)],
            back_send.at[target],
            back_recv.at[source],
            core * group_count + target,
        )

    gating = gate_in[pl.ds(t_ref[0], 1), :]
    patches = group_count // PARTS
    for part in range(PARTS):

        @pl.loop(0, column_pieces)
        def _(index):
            column_copy(part, place, column_source(index, 1 - side)).wait_recv()

        tiles = [pieces[part, g, :part_rows] for g in range(group_count)]
        for pair in range(group_count // 2):
            even = pieces[part, 2 * pair, part_rows:]
            upper = pieces[part, 2 * pair + 1, part_rows:]
            top = jnp.where(odd_low, even, swap_halves(upper))
            bottom = jnp.where(odd_low, swap_halves(even), upper)
            tiles.append(jnp.concatenate([top, bottom], 0))
        attended = jnp.concatenate(tiles, 1)
        projected = jnp.dot(attended, weight[...], preferred_element_type=jnp.float32)
        product[part * patches : (part + 1) * patches] = (
            (projected * gating).astype(product.dtype).reshape(patches, rows, columns)
        )

        @pl.loop(0, patches)
        def _(step):
            target = part * patches + (position + step) % patches

            @pl.when(core * group_count + target != me)
            def _():
                back_copy(target, chip).start()

        @pl.when((core == block) & (position // patches == part))
        def _():
            pltpu.make_async_copy(
                product.at[position],
                out_ref.at[:, chip_columns],
                back_recv.at[chip],
            ).start()

    @pl.loop(1, group_count)
    def _(step):
        fresh_copy((position + step) % group_count, position).wait_send()

    @pl.loop(1, devices)
    def _(step):
        stale_copy((me + step) % devices, me).wait_send()

    weight_copy.wait_send()

    for part in range(PARTS):

        column_copy(part, gate, position).wait_send()
        across_copy(part).wait_send()
        column_copy(part, mate, position).wait_send()

        @pl.when(core != block)
        def _():
            column_copy(part, place, position).wait_send()

        @pl.loop(0, column_pieces)
        def _(index):
            source = column_source(index, side)

            @pl.when(at_gate)
            def _():
                far_copy(part, source, index).wait_send()

            @pl.when(elsewhere | (index // CORES != place % 2))
            def _():
                forward_copy(part, source, index).wait_send()

    @pl.loop(0, group_count)
    def _(target):
        @pl.when(core * group_count + target != me)
        def _():
            back_copy(target, chip).wait_send()

    @pl.loop(0, chips)
    def _(source):
        back_copy(position, source).wait_recv()


def fused_body(
    queries,
    fresh_keys,
    fresh_values,
    stale_keys,
    stale_values,
    text_keys,
    text_values,
    out_weight,
    gate_table,
    timestep,
):
    devices = lax.axis_size("patch")
    chips = devices // CORES
    group_count = chips
    rows, width = queries.shape
    block_rows = group_count * rows
    piece_rows = (block_rows + block_rows // 2) // PARTS
    text_rows = text_keys.shape[0]
    padded = -(-text_rows // LANES) * LANES
    depth, part_columns = out_weight.shape
    columns = CORES * part_columns
    bf16 = jnp.bfloat16
    dma = pltpu.SemaphoreType.DMA
    anywhere = pl.BlockSpec(memory_space=pl.ANY)
    return pl.pallas_call(
        functools.partial(fused_kernel, devices),
        out_shape=pltpu.VMEM((rows, part_columns * devices), bf16),
        in_specs=[anywhere] * 9 + [pl.BlockSpec(memory_space=pltpu.SMEM)],
        out_specs=pl.BlockSpec(memory_space=pltpu.VMEM),
        scratch_shapes=[
            pltpu.VMEM((5, rows, width), bf16),
            pltpu.VMEM((4, text_rows, LANES), bf16),
            pltpu.VMEM((gate_table.shape[0], columns), jnp.float32),
            pltpu.VMEM((columns, depth), bf16),
            pltpu.VMEM((depth, columns), bf16),
            pltpu.VMEM((group_count, 5, rows, LANES), bf16),
            pltpu.VMEM((group_count, 3, rows, LANES), bf16),
            pltpu.VMEM((5, block_rows, LANES), bf16),
            pltpu.VMEM((2, 3, block_rows, LANES), bf16),
            pltpu.VMEM((3, padded, LANES), bf16),
            pltpu.VMEM((PARTS, piece_rows, LANES), bf16),
            pltpu.VMEM((PARTS, group_count, piece_rows, LANES), bf16),
            pltpu.VMEM((group_count, rows, columns), bf16),
            dma((11,)),
            dma((group_count,)),
            dma((group_count,)),
            dma((devices,)),
            dma((devices,)),
            dma,
            dma,
            dma((PARTS, chips // 2)),
            dma((PARTS,)),
            dma((PARTS, group_count // 2)),
            dma((PARTS, group_count // 2)),
            dma((PARTS, group_count)),
            dma((group_count,)),
            dma((chips,)),
        ],
        compiler_params=pltpu.CompilerParams(collective_id=0, has_side_effects=True),
    )(
        queries,
        fresh_keys,
        fresh_values,
        stale_keys,
        stale_values,
        text_keys,
        text_values,
        out_weight.T,
        gate_table,
        timestep,
    )


def solution(mesh):
    in_specs = (
        P(("groups", "patch"), None),
        P(("groups", "patch"), None),
        P(("groups", "patch"), None),
        P(("groups", "patch"), None),
        P(("groups", "patch"), None),
        P("groups", None),
        P("groups", None),
        P(None, "patch"),
        P(),
        P("groups"),
    )
    out_specs = P(("groups", "patch"), None)
    chosen = fused_body if fused_fits(mesh) else body
    return jax.shard_map(chosen, mesh=mesh, in_specs=in_specs, out_specs=out_specs, check_vma=False)
```

```python
import functools
import math

import jax
import jax.numpy as jnp
from jax import lax
from jax.experimental import pallas as pl
from jax.experimental.pallas import tpu as pltpu
from jax.sharding import PartitionSpec as P

HEAD_DIM = 64
HEADS = 24


def from_behind(shard, axis, by):
    peers = lax.axis_size(axis)
    return lax.ppermute(shard, axis, [(i, (i + by) % peers) for i in range(peers)])


def pick_group(stacked, position):
    return lax.dynamic_index_in_dim(stacked, position, 0, keepdims=False)


def by_group(matrix, group_count):
    width = matrix.shape[1] // group_count
    return matrix.reshape(matrix.shape[0], group_count, width).transpose(1, 0, 2)


def gather_block(stacked, group_count, position):
    received = [pick_group(stacked, position)]
    for step_size in range(1, group_count):
        payload = pick_group(stacked, (position + step_size) % group_count)
        arrived = []
        for offset_by in (step_size, step_size - group_count):
            arrived.append(from_behind(payload, "patch", offset_by))
        received.append(jnp.where(position >= step_size, arrived[0], arrived[1]))
    ordered = jnp.stack(received, 0)
    order = (position - jnp.arange(group_count, dtype=jnp.int32)) % group_count
    return jnp.take(ordered, order, axis=0)


def return_block(stacked, group_count, position):
    received = [pick_group(stacked, position)]
    for step_size in range(1, group_count):
        payload = pick_group(stacked, (position + step_size) % group_count)
        arrived = []
        for offset_by in (step_size, step_size - group_count):
            arrived.append(from_behind(payload, "patch", offset_by))
        received.append(jnp.where(position >= step_size, arrived[0], arrived[1]))
    ordered = jnp.stack(received, 0)
    order = (position - jnp.arange(group_count, dtype=jnp.int32)) % group_count
    return jnp.take(ordered, order, axis=0)


def body(
    queries,
    fresh_keys,
    fresh_values,
    stale_keys,
    stale_values,
    text_keys,
    text_values,
    out_weight,
    gate_table,
    timestep,
):
    row_count = queries.shape[0]
    head_count = HEADS
    head_width = HEAD_DIM
    scaling = head_width ** (-0.5)
    group_count = math.gcd(head_count, 8)
    group_heads = head_count // group_count
    group_width = group_heads * head_width
    device_count = lax.axis_size("patch")
    position = lax.axis_index("patch") % group_count
    block_first = lax.axis_index("patch") // group_count * group_count
    local_stack = jnp.stack(
        [
            by_group(queries, group_count),
            by_group(fresh_keys, group_count),
            by_group(fresh_values, group_count),
        ],
        1,
    )
    block_stack = gather_block(local_stack, group_count, position)
    block_rows_count = group_count * row_count
    block_query = block_stack[:, 0].reshape(block_rows_count, group_heads, head_width)
    block_keys = block_stack[:, 1].reshape(block_rows_count, group_heads, head_width)
    block_values = block_stack[:, 2].reshape(block_rows_count, group_heads, head_width)
    spread_keys = jnp.tile(by_group(stale_keys, group_count), (device_count // group_count, 1, 1))
    spread_values = jnp.tile(
        by_group(stale_values, group_count), (device_count // group_count, 1, 1)
    )
    every_keys, every_values = (
        lax.all_to_all(spread_keys, "patch", split_axis=0, concat_axis=0, tiled=True),
        lax.all_to_all(spread_values, "patch", split_axis=0, concat_axis=0, tiled=True),
    )
    every_keys = every_keys.reshape(device_count * row_count, group_heads, head_width)
    every_values = every_values.reshape(device_count * row_count, group_heads, head_width)
    text_k = pick_group(by_group(text_keys, group_count), position).reshape(
        -1, group_heads, head_width
    )
    text_v = pick_group(by_group(text_values, group_count), position).reshape(
        -1, group_heads, head_width
    )
    query_patch = jnp.arange(block_rows_count, dtype=jnp.int32) // row_count
    stale_patch = jnp.arange(device_count * row_count, dtype=jnp.int32) // row_count
    stale_mask = stale_patch[None, :] != (block_first + query_patch)[:, None]
    fresh_mask = query_patch[None, :] == query_patch[:, None]

    def scored(key_block):
        return (
            jnp.einsum("qhd,khd->qhk", block_query, key_block, preferred_element_type=jnp.float32)
            * scaling
        )

    text_scores = scored(text_k)
    fresh_scores = jnp.where(fresh_mask[:, None, :], scored(block_keys), -1e30)
    stale_scores = jnp.where(stale_mask[:, None, :], scored(every_keys), -1e30)
    highest = jnp.maximum(
        jnp.maximum(jnp.max(text_scores, -1), jnp.max(fresh_scores, -1)), jnp.max(stale_scores, -1)
    )
    text_expo = jnp.exp(text_scores - highest[..., None])
    fresh_expo = jnp.exp(fresh_scores - highest[..., None])
    stale_expo = jnp.exp(stale_scores - highest[..., None])
    total = jnp.sum(text_expo, -1) + jnp.sum(fresh_expo, -1) + jnp.sum(stale_expo, -1)

    def weigh_block(expo, value_block):
        return jnp.einsum(
            "qhk,khd->qhd",
            expo.astype(jnp.bfloat16),
            value_block,
            preferred_element_type=jnp.float32,
        )

    weighted = (
        weigh_block(text_expo, text_v)
        + weigh_block(fresh_expo, block_values)
        + weigh_block(stale_expo, every_values)
    )
    block_out = (
        (weighted / total[..., None])
        .reshape(group_count, row_count, group_width)
        .astype(jnp.bfloat16)
    )
    home = return_block(block_out, group_count, position)
    attended = home.transpose(1, 0, 2).reshape(row_count, head_count * head_width)
    projected = jnp.dot(
        attended,
        lax.all_gather(out_weight, "patch", axis=1, tiled=True),
        preferred_element_type=jnp.float32,
    )
    selector = (jnp.arange(gate_table.shape[0], dtype=jnp.int32) == timestep[0]).astype(jnp.float32)
    gating = jnp.dot(selector, gate_table, precision=lax.Precision.HIGHEST)
    return (projected * gating[None, :]).astype(jnp.bfloat16)


LANES = 128
CORES = 2
LINES = 4
HALVES = 1
PARTS = 4
NEVER = -1e30
MESH = pl.DeviceIdType.MESH


def fused_fits(mesh):
    chips = mesh.shape["patch"] // CORES
    return (
        2 * HEAD_DIM == LANES
        and mesh.shape["patch"] % (2 * CORES) == 0
        and HEADS == 3 * chips
        and chips == math.gcd(HEADS, 8)
        and chips == 4 * CORES
    )


def swap_halves(tile):
    return pltpu.roll(tile.astype(jnp.float32), HEAD_DIM, 1).astype(tile.dtype)


def low_lanes(rows):
    return lax.broadcasted_iota(jnp.int32, (rows, LANES), 1) < HEAD_DIM


def odd_pair(first, second, upper):
    low = low_lanes(first.shape[0])
    if upper:
        return jnp.where(low, swap_halves(first), second)
    return jnp.where(low, first, swap_halves(second))


def score(query, keys):
    return lax.dot_general(query, keys, (((1,), (1,)), ((), ())), preferred_element_type=jnp.float32)


def weigh(probs, values):
    return jnp.dot(probs, values, preferred_element_type=jnp.float32)


def fused_kernel(
    devices,
    q_ref,
    kf_ref,
    vf_ref,
    ks_ref,
    vs_ref,
    tk_ref,
    tv_ref,
    w_ref,
    g_ref,
    t_ref,
    out_ref,
    rows_in,
    text_in,
    gate_in,
    weights,
    weight,
    send,
    near,
    away,
    text,
    piece,
    pieces,
    product,
    load_sem,
    seen,
    near_send,
    near_recv,
    away_send,
    away_recv,
    weight_send,
    weight_recv,
    piece_send,
    piece_across,
    piece_forward,
    piece_far,
    piece_recv,
    back_send,
    back_recv,
):
    groups = lax.axis_index("groups")
    me = lax.axis_index("patch")
    chips = devices // CORES
    group_count = chips
    rows = q_ref.shape[0]
    block_rows = group_count * rows
    text_rows = tk_ref.shape[0]
    part_columns = w_ref.shape[0]
    columns = CORES * part_columns
    chip, core = me // CORES, me % CORES
    block, position = me // group_count, me % group_count
    partner = me + 1 - 2 * core
    side, place = chip % 2, chip // 2
    places = chips // 2
    odd_tile = group_count + position // 2

    def device(index):
        return (groups, index)

    def remote(src, dst, send, recv, index):
        return pltpu.make_async_remote_copy(
            src_ref=src,
            dst_ref=dst,
            send_sem=send,
            recv_sem=recv,
            device_id=device(index),
            device_id_type=MESH,
        )

    def weight_rows(of_core):
        start = pl.multiple_of(of_core * part_columns, part_columns)
        return weights.at[pl.ds(start, part_columns), :]

    loads = [
        pltpu.make_async_copy(ref, rows_in.at[i], load_sem.at[i])
        for i, ref in enumerate((q_ref, kf_ref, vf_ref, ks_ref, vs_ref))
    ]
    for load in loads:
        load.start()

    barrier = pltpu.get_barrier_semaphore()
    has_below, has_above = place > 0, place < places - 1

    def greet(index):
        pl.semaphore_signal(barrier, inc=1, device_id=device(index), device_id_type=MESH)

    @pl.when(has_above)
    def _():
        greet(me + LINES)

    @pl.when(has_below)
    def _():
        greet(me - LINES)

    for step in range(1, LINES):
        greet(place * LINES + (me + step) % LINES)

    full_lanes = pl.ds(pl.multiple_of(position * LANES, LANES), LANES)
    odd_lanes = pl.ds(pl.multiple_of(odd_tile * LANES, LANES), LANES)
    for i, (ref, lanes) in enumerate(
        ((tk_ref, full_lanes), (tv_ref, full_lanes), (tk_ref, odd_lanes), (tv_ref, odd_lanes))
    ):
        loads.append(pltpu.make_async_copy(ref.at[:, lanes], text_in.at[i], load_sem.at[5 + i]))
    chip_columns = pl.ds(pl.multiple_of(chip * columns, LANES), columns)
    loads.append(pltpu.make_async_copy(g_ref.at[:, chip_columns], gate_in, load_sem.at[9]))
    loads.append(pltpu.make_async_copy(w_ref, weight_rows(core), load_sem.at[10]))
    for load in loads[5:]:
        load.start()

    pl.semaphore_wait(
        barrier, LINES - 1 + has_below.astype(jnp.int32) + has_above.astype(jnp.int32)
    )

    def tell(index, about):
        pl.semaphore_signal(seen.at[about], inc=1, device_id=device(index), device_id_type=MESH)

    @pl.when(has_above)
    def _():
        tell(me + LINES, place)

    @pl.when(has_below)
    def _():
        tell(me - LINES, place)

    def hear(other):
        pl.semaphore_wait(seen.at[other], 1)

        @pl.when((other < place) & has_above)
        def _():
            tell(me + LINES, other)

        @pl.when((other > place) & has_below)
        def _():
            tell(me - LINES, other)

    @pl.when(has_below & has_above)
    def _():
        @pl.loop(0, place)
        def _(step):
            hear(place - 1 - step)

        @pl.when(block == 1)
        def _():
            @pl.loop(place + 1, places)
            def _(other):
                hear(other)

    for load in loads[:5]:
        load.wait()
    for g in range(group_count):
        own = slice(g * LANES, (g + 1) * LANES)
        tile = group_count + g // 2
        odd = slice(tile * LANES, (tile + 1) * LANES)
        upper = g % 2 == 1
        half_rows = rows // 2
        sent = (
            rows_in[3, :, own],
            rows_in[4, :, own],
            odd_pair(rows_in[3, :, odd], rows_in[4, :, odd], upper),
            rows_in[0, :, own],
            rows_in[1, :, own],
            rows_in[2, :, own],
            odd_pair(rows_in[1, :, odd], rows_in[2, :, odd], upper),
            odd_pair(rows_in[0, :half_rows, odd], rows_in[0, half_rows:, odd], upper),
        )
        for i, tile_rows in enumerate(sent):
            send[g, i * rows : i * rows + tile_rows.shape[0]] = tile_rows

    def near_copy(target, source):
        return remote(
            send.at[target],
            near.at[source],
            near_send.at[target],
            near_recv.at[source],
            block * group_count + target,
        )

    def away_copy(target, source):
        return remote(
            send.at[target, pl.ds(0, 3 * rows)],
            away.at[source],
            away_send.at[target],
            away_recv.at[source],
            (1 - block) * group_count + target,
        )

    def send_plane(other):
        @pl.loop(0, LINES)
        def _(step):
            target = other % 2 * LINES + (me + step) % LINES

            @pl.when(other // 2 == block)
            def _():
                near_copy(target, position).start()

            @pl.when(other // 2 != block)
            def _():
                away_copy(target, position).start()

    def send_here():
        @pl.loop(1, LINES)
        def _(step):
            near_copy(place % 2 * LINES + (me + step) % LINES, position).start()

    @pl.when(block == 0)
    def _():
        send_here()

        @pl.when(has_below)
        def _():
            send_plane(place - 1)

        @pl.loop(place + 1, places)
        def _(other):
            hear(other)
            send_plane(other)

    @pl.when(block == 1)
    def _():
        @pl.when(jnp.logical_not(has_above))
        def _():
            @pl.loop(0, place)
            def _(step):
                hear(place - 1 - step)

        @pl.when(has_above)
        def _():
            send_plane(2 * block + 1 - place % 2)
            send_plane(1)
            send_plane(0)
            send_here()

        @pl.when(jnp.logical_not(has_above))
        def _():
            send_plane(0)
            send_plane(1)
            send_plane(2 * block + 1 - place % 2)
            send_here()

    pltpu.make_async_copy(send.at[position], near.at[position], near_recv.at[position]).start()
    weight_copy = remote(w_ref, weight_rows(core), weight_send, weight_recv, partner)
    weight_copy.start()

    for load in loads[5:9]:
        load.wait()
    text[...] = jnp.zeros_like(text)
    text[0, :text_rows] = text_in[0]
    text[1, :text_rows] = text_in[1]
    text[2, :text_rows] = jnp.where(
        position % 2 == 1,
        odd_pair(text_in[2], text_in[3], True),
        odd_pair(text_in[2], text_in[3], False),
    )
    loads[9].wait()
    loads[10].wait()
    remote(w_ref, weight_rows(1 - core), weight_send, weight_recv, partner).wait_recv()
    depth = w_ref.shape[1]
    chunk = 2 * LANES

    @pl.loop(0, depth // chunk)
    def _(step):
        at = pl.ds(pl.multiple_of(step * chunk, chunk), chunk)
        weight[at, :] = weights[:, at].T

    scaling = HEAD_DIM**-0.5
    half = block_rows // HALVES
    part_rows = block_rows // PARTS
    odd_rows = part_rows // 2
    padded = text.shape[1]

    def same_patch(stacked):
        query = lax.broadcasted_iota(jnp.int32, (stacked * half, 1), 0) % half // rows
        key = lax.broadcasted_iota(jnp.int32, (1, half), 1) // rows
        return query == key

    def lane_sums(expo):
        sums = expo[:, :LANES]
        for first in range(LANES, expo.shape[1], LANES):
            sums = sums + expo[:, first : first + LANES]
        return sums

    def finish(state, scores, values):
        highest, sums, weighted = state
        peak = jnp.maximum(highest, jnp.max(scores, -1, keepdims=True))
        fade = jnp.exp(highest - peak)
        expo = jnp.exp(scores - peak)
        total = jnp.sum(sums * fade + lane_sums(expo), -1, keepdims=True)
        weighted = weighted * fade + weigh(expo.astype(jnp.bfloat16), values)
        return weighted / total

    @pl.loop(0, group_count)
    def _(source):
        near_copy(position, source).wait_recv()

    def tiles_of(ref, index, first=0, last=group_count):
        at = slice(index * rows, (index + 1) * rows)
        return jnp.concatenate([ref[source, at] for source in range(first, last)], 0)

    low = low_lanes(half)
    half_low = low_lanes(rows // 2)
    per_half = group_count // HALVES
    units = []
    for part in range(HALVES):
        mine = (part * per_half, (part + 1) * per_half)
        pair_query = tiles_of(near, 3, *mine) * jnp.asarray(scaling, near.dtype)
        nothing = jnp.zeros_like(pair_query)
        both = jnp.concatenate(
            [jnp.where(low, pair_query, nothing), jnp.where(low, nothing, pair_query)], 0
        )
        odd_query = []
        for source in range(*mine):
            packed = near[source, 7 * rows :]
            for each in (packed, swap_halves(packed)):
                odd_query.append(jnp.where(half_low, each, jnp.zeros_like(each)))
        odd_query = jnp.concatenate(odd_query, 0) * jnp.asarray(scaling, near.dtype)
        units.append((part, 2, (4, 5, 0, 1), text[0], text[1], both))
        units.append((part, 1, (6, 6, 2, 2), text[2], text[2], odd_query))

    states = []
    last = padded - LANES
    absent = lax.broadcasted_iota(jnp.int32, (1, LANES), 1) >= text_rows - last
    for part, stacked, kinds, text_key, text_value, query in units:
        mine = (part * per_half, (part + 1) * per_half)
        new_key, new_value, old_key, old_value = (tiles_of(near, kind, *mine) for kind in kinds)
        scores = score(query, jnp.concatenate([text_key, old_key, new_key], 0))
        same = same_patch(stacked)
        mixed = jnp.where(same, scores[:, padded + half :], scores[:, padded : padded + half])
        scores = jnp.concatenate(
            [scores[:, :last], jnp.where(absent, NEVER, scores[:, last:padded]), mixed], 1
        )
        peak = jnp.max(scores, -1, keepdims=True)
        expo = jnp.exp(scores - peak)
        mixed = expo[:, padded:]
        probs = [expo[:, :padded], jnp.where(same, 0.0, mixed), jnp.where(same, mixed, 0.0)]
        probs = jnp.concatenate([each.astype(jnp.bfloat16) for each in probs], 1)
        values = jnp.concatenate([text_value, old_value, new_value], 0)
        states.append((peak, lane_sums(expo), weigh(probs, values)))

    @pl.loop(0, group_count)
    def _(source):
        away_copy(position, source).wait_recv()

    def column_copy(part, target_place, source):
        return remote(
            piece.at[part],
            pieces.at[part, source],
            piece_send.at[part, target_place],
            piece_recv.at[part, source],
            (target_place * 2 + side) * CORES + block,
        )

    def across_copy(part):
        return remote(
            piece.at[part],
            pieces.at[part, position],
            piece_across.at[part],
            piece_recv.at[part, position],
            (place * 2 + 1 - side) * CORES + block,
        )

    def forward_copy(part, source, index):
        return remote(
            pieces.at[part, source],
            pieces.at[part, source],
            piece_forward.at[part, index],
            piece_recv.at[part, source],
            (place * 2 + 1 - side) * CORES + core,
        )

    def far_copy(part, source, index):
        return remote(
            pieces.at[part, source],
            pieces.at[part, source],
            piece_far.at[part, index],
            piece_recv.at[part, source],
            ((1 - core) * (places - 1) * 2 + side) * CORES + core,
        )

    mate = 2 * block + 1 - place % 2
    gate = 2 - block
    at_gate = place == 2 - core
    elsewhere = place // 2 != core

    part_low = low_lanes(part_rows)
    odd_low = low_lanes(odd_rows)
    done = []
    for part in range(PARTS):
        if part % (PARTS // HALVES) == 0:
            done = []
            first_unit = 2 * (part * HALVES // PARTS)
            for i in (first_unit, first_unit + 1):
                _, _, kinds, _, _, query = units[i]
                key, value = (tiles_of(away, kind) for kind in kinds[2:])
                done.append(finish(states[i], score(query, key), value))
        at = part % (PARTS // HALVES) * part_rows
        piece[part, :part_rows] = jnp.where(
            part_low, done[0][at : at + part_rows], done[0][half + at : half + at + part_rows]
        ).astype(piece.dtype)
        piece[part, part_rows:] = jnp.where(
            odd_low,
            pltpu.roll(done[1][at : at + odd_rows], HEAD_DIM, 1),
            done[1][at + odd_rows : at + part_rows],
        ).astype(piece.dtype)

        column_copy(part, gate, position).start()
        across_copy(part).start()
        column_copy(part, mate, position).start()

        @pl.when(core == block)
        def _():
            pltpu.make_async_copy(
                piece.at[part], pieces.at[part, position], piece_recv.at[part, position]
            ).start()

        @pl.when(core != block)
        def _():
            column_copy(part, place, position).start()

    def column_source(index, of_side):
        return index // CORES * 2 * CORES + of_side * CORES + index % CORES

    column_pieces = group_count // 2

    for part in range(PARTS):

        @pl.loop(0, column_pieces)
        def _(index):
            index = (index + (1 - core) * CORES) % column_pieces
            source = column_source(index, side)
            column_copy(part, place, source).wait_recv()

            @pl.when(at_gate)
            def _():
                far_copy(part, source, index).start()

            @pl.when(elsewhere | (index // CORES != place % 2))
            def _():
                forward_copy(part, source, index).start()

    def back_copy(target, source):
        return remote(
            product.at[target],
            out_ref.at[:, pl.ds(pl.multiple_of(source * columns, LANES), columns)],
            back_send.at[target],
            back_recv.at[source],
            core * group_count + target,
        )

    gating = gate_in[pl.ds(t_ref[0], 1), :]
    patches = group_count // PARTS
    for part in range(PARTS):

        @pl.loop(0, column_pieces)
        def _(index):
            column_copy(part, place, column_source(index, 1 - side)).wait_recv()

        tiles = [pieces[part, g, :part_rows] for g in range(group_count)]
        for pair in range(group_count // 2):
            even = pieces[part, 2 * pair, part_rows:]
            upper = pieces[part, 2 * pair + 1, part_rows:]
            top = jnp.where(odd_low, even, swap_halves(upper))
            bottom = jnp.where(odd_low, swap_halves(even), upper)
            tiles.append(jnp.concatenate([top, bottom], 0))
        attended = jnp.concatenate(tiles, 1)
        projected = jnp.dot(attended, weight[...], preferred_element_type=jnp.float32)
        product[part * patches : (part + 1) * patches] = (
            (projected * gating).astype(product.dtype).reshape(patches, rows, columns)
        )

        @pl.loop(0, patches)
        def _(step):
            target = part * patches + (position + step) % patches

            @pl.when(core * group_count + target != me)
            def _():
                back_copy(target, chip).start()

        @pl.when((core == block) & (position // patches == part))
        def _():
            pltpu.make_async_copy(
                product.at[position],
                out_ref.at[:, chip_columns],
                back_recv.at[chip],
            ).start()

    @pl.loop(1, group_count)
    def _(step):
        near_copy((position + step) % group_count, position).wait_send()

    @pl.loop(0, group_count)
    def _(target):
        away_copy(target, position).wait_send()

    weight_copy.wait_send()

    for part in range(PARTS):

        column_copy(part, gate, position).wait_send()
        across_copy(part).wait_send()
        column_copy(part, mate, position).wait_send()

        @pl.when(core != block)
        def _():
            column_copy(part, place, position).wait_send()

        @pl.loop(0, column_pieces)
        def _(index):
            source = column_source(index, side)

            @pl.when(at_gate)
            def _():
                far_copy(part, source, index).wait_send()

            @pl.when(elsewhere | (index // CORES != place % 2))
            def _():
                forward_copy(part, source, index).wait_send()

    @pl.loop(0, group_count)
    def _(target):
        @pl.when(core * group_count + target != me)
        def _():
            back_copy(target, chip).wait_send()

    @pl.loop(0, chips)
    def _(source):
        back_copy(position, source).wait_recv()


def fused_body(
    queries,
    fresh_keys,
    fresh_values,
    stale_keys,
    stale_values,
    text_keys,
    text_values,
    out_weight,
    gate_table,
    timestep,
):
    devices = lax.axis_size("patch")
    chips = devices // CORES
    group_count = chips
    rows, width = queries.shape
    block_rows = group_count * rows
    piece_rows = (block_rows + block_rows // 2) // PARTS
    text_rows = text_keys.shape[0]
    padded = -(-text_rows // LANES) * LANES
    depth, part_columns = out_weight.shape
    columns = CORES * part_columns
    bf16 = jnp.bfloat16
    dma = pltpu.SemaphoreType.DMA
    anywhere = pl.BlockSpec(memory_space=pl.ANY)
    return pl.pallas_call(
        functools.partial(fused_kernel, devices),
        out_shape=pltpu.VMEM((rows, part_columns * devices), bf16),
        in_specs=[anywhere] * 9 + [pl.BlockSpec(memory_space=pltpu.SMEM)],
        out_specs=pl.BlockSpec(memory_space=pltpu.VMEM),
        scratch_shapes=[
            pltpu.VMEM((5, rows, width), bf16),
            pltpu.VMEM((4, text_rows, LANES), bf16),
            pltpu.VMEM((gate_table.shape[0], columns), jnp.float32),
            pltpu.VMEM((columns, depth), bf16),
            pltpu.VMEM((depth, columns), bf16),
            pltpu.VMEM((group_count, 7 * rows + rows // 2, LANES), bf16),
            pltpu.VMEM((group_count, 7 * rows + rows // 2, LANES), bf16),
            pltpu.VMEM((group_count, 3 * rows, LANES), bf16),
            pltpu.VMEM((3, padded, LANES), bf16),
            pltpu.VMEM((PARTS, piece_rows, LANES), bf16),
            pltpu.VMEM((PARTS, group_count, piece_rows, LANES), bf16),
            pltpu.VMEM((group_count, rows, columns), bf16),
            dma((11,)),
            pltpu.SemaphoreType.REGULAR((chips // 2,)),
            dma((group_count,)),
            dma((group_count,)),
            dma((group_count,)),
            dma((group_count,)),
            dma,
            dma,
            dma((PARTS, chips // 2)),
            dma((PARTS,)),
            dma((PARTS, group_count // 2)),
            dma((PARTS, group_count // 2)),
            dma((PARTS, group_count)),
            dma((group_count,)),
            dma((chips,)),
        ],
        compiler_params=pltpu.CompilerParams(collective_id=0, has_side_effects=True),
    )(
        queries,
        fresh_keys,
        fresh_values,
        stale_keys,
        stale_values,
        text_keys,
        text_values,
        out_weight.T,
        gate_table,
        timestep,
    )


def solution(mesh):
    in_specs = (
        P(("groups", "patch"), None),
        P(("groups", "patch"), None),
        P(("groups", "patch"), None),
        P(("groups", "patch"), None),
        P(("groups", "patch"), None),
        P("groups", None),
        P("groups", None),
        P(None, "patch"),
        P(),
        P("groups"),
    )
    out_specs = P(("groups", "patch"), None)
    chosen = fused_body if fused_fits(mesh) else body
    return jax.shard_map(chosen, mesh=mesh, in_specs=in_specs, out_specs=out_specs, check_vma=False)
```

```python
import functools
import math

import jax
import jax.numpy as jnp
from jax import lax
from jax.experimental import pallas as pl
from jax.experimental.pallas import tpu as pltpu
from jax.sharding import PartitionSpec as P

HEAD_DIM = 64
HEADS = 24


def from_behind(shard, axis, by):
    peers = lax.axis_size(axis)
    return lax.ppermute(shard, axis, [(i, (i + by) % peers) for i in range(peers)])


def pick_group(stacked, position):
    return lax.dynamic_index_in_dim(stacked, position, 0, keepdims=False)


def by_group(matrix, group_count):
    width = matrix.shape[1] // group_count
    return matrix.reshape(matrix.shape[0], group_count, width).transpose(1, 0, 2)


def gather_block(stacked, group_count, position):
    received = [pick_group(stacked, position)]
    for step_size in range(1, group_count):
        payload = pick_group(stacked, (position + step_size) % group_count)
        arrived = []
        for offset_by in (step_size, step_size - group_count):
            arrived.append(from_behind(payload, "patch", offset_by))
        received.append(jnp.where(position >= step_size, arrived[0], arrived[1]))
    ordered = jnp.stack(received, 0)
    order = (position - jnp.arange(group_count, dtype=jnp.int32)) % group_count
    return jnp.take(ordered, order, axis=0)


def return_block(stacked, group_count, position):
    received = [pick_group(stacked, position)]
    for step_size in range(1, group_count):
        payload = pick_group(stacked, (position + step_size) % group_count)
        arrived = []
        for offset_by in (step_size, step_size - group_count):
            arrived.append(from_behind(payload, "patch", offset_by))
        received.append(jnp.where(position >= step_size, arrived[0], arrived[1]))
    ordered = jnp.stack(received, 0)
    order = (position - jnp.arange(group_count, dtype=jnp.int32)) % group_count
    return jnp.take(ordered, order, axis=0)


def body(
    queries,
    fresh_keys,
    fresh_values,
    stale_keys,
    stale_values,
    text_keys,
    text_values,
    out_weight,
    gate_table,
    timestep,
):
    row_count = queries.shape[0]
    head_count = HEADS
    head_width = HEAD_DIM
    scaling = head_width ** (-0.5)
    group_count = math.gcd(head_count, 8)
    group_heads = head_count // group_count
    group_width = group_heads * head_width
    device_count = lax.axis_size("patch")
    position = lax.axis_index("patch") % group_count
    block_first = lax.axis_index("patch") // group_count * group_count
    local_stack = jnp.stack(
        [
            by_group(queries, group_count),
            by_group(fresh_keys, group_count),
            by_group(fresh_values, group_count),
        ],
        1,
    )
    block_stack = gather_block(local_stack, group_count, position)
    block_rows_count = group_count * row_count
    block_query = block_stack[:, 0].reshape(block_rows_count, group_heads, head_width)
    block_keys = block_stack[:, 1].reshape(block_rows_count, group_heads, head_width)
    block_values = block_stack[:, 2].reshape(block_rows_count, group_heads, head_width)
    spread_keys = jnp.tile(by_group(stale_keys, group_count), (device_count // group_count, 1, 1))
    spread_values = jnp.tile(
        by_group(stale_values, group_count), (device_count // group_count, 1, 1)
    )
    every_keys, every_values = (
        lax.all_to_all(spread_keys, "patch", split_axis=0, concat_axis=0, tiled=True),
        lax.all_to_all(spread_values, "patch", split_axis=0, concat_axis=0, tiled=True),
    )
    every_keys = every_keys.reshape(device_count * row_count, group_heads, head_width)
    every_values = every_values.reshape(device_count * row_count, group_heads, head_width)
    text_k = pick_group(by_group(text_keys, group_count), position).reshape(
        -1, group_heads, head_width
    )
    text_v = pick_group(by_group(text_values, group_count), position).reshape(
        -1, group_heads, head_width
    )
    query_patch = jnp.arange(block_rows_count, dtype=jnp.int32) // row_count
    stale_patch = jnp.arange(device_count * row_count, dtype=jnp.int32) // row_count
    stale_mask = stale_patch[None, :] != (block_first + query_patch)[:, None]
    fresh_mask = query_patch[None, :] == query_patch[:, None]

    def scored(key_block):
        return (
            jnp.einsum("qhd,khd->qhk", block_query, key_block, preferred_element_type=jnp.float32)
            * scaling
        )

    text_scores = scored(text_k)
    fresh_scores = jnp.where(fresh_mask[:, None, :], scored(block_keys), -1e30)
    stale_scores = jnp.where(stale_mask[:, None, :], scored(every_keys), -1e30)
    highest = jnp.maximum(
        jnp.maximum(jnp.max(text_scores, -1), jnp.max(fresh_scores, -1)), jnp.max(stale_scores, -1)
    )
    text_expo = jnp.exp(text_scores - highest[..., None])
    fresh_expo = jnp.exp(fresh_scores - highest[..., None])
    stale_expo = jnp.exp(stale_scores - highest[..., None])
    total = jnp.sum(text_expo, -1) + jnp.sum(fresh_expo, -1) + jnp.sum(stale_expo, -1)

    def weigh_block(expo, value_block):
        return jnp.einsum(
            "qhk,khd->qhd",
            expo.astype(jnp.bfloat16),
            value_block,
            preferred_element_type=jnp.float32,
        )

    weighted = (
        weigh_block(text_expo, text_v)
        + weigh_block(fresh_expo, block_values)
        + weigh_block(stale_expo, every_values)
    )
    block_out = (
        (weighted / total[..., None])
        .reshape(group_count, row_count, group_width)
        .astype(jnp.bfloat16)
    )
    home = return_block(block_out, group_count, position)
    attended = home.transpose(1, 0, 2).reshape(row_count, head_count * head_width)
    projected = jnp.dot(
        attended,
        lax.all_gather(out_weight, "patch", axis=1, tiled=True),
        preferred_element_type=jnp.float32,
    )
    selector = (jnp.arange(gate_table.shape[0], dtype=jnp.int32) == timestep[0]).astype(jnp.float32)
    gating = jnp.dot(selector, gate_table, precision=lax.Precision.HIGHEST)
    return (projected * gating[None, :]).astype(jnp.bfloat16)


LANES = 128
CORES = 2
LINES = 4
HALVES = 1
PARTS = 4
NEVER = -1e30
MESH = pl.DeviceIdType.MESH


def fused_fits(mesh):
    chips = mesh.shape["patch"] // CORES
    return (
        2 * HEAD_DIM == LANES
        and mesh.shape["patch"] % (2 * CORES) == 0
        and HEADS == 3 * chips
        and chips == math.gcd(HEADS, 8)
        and chips == 4 * CORES
    )


def swap_halves(tile):
    return pltpu.roll(tile.astype(jnp.float32), HEAD_DIM, 1).astype(tile.dtype)


def low_lanes(rows):
    return lax.broadcasted_iota(jnp.int32, (rows, LANES), 1) < HEAD_DIM


def odd_pair(first, second, upper):
    low = low_lanes(first.shape[0])
    if upper:
        return jnp.where(low, swap_halves(first), second)
    return jnp.where(low, first, swap_halves(second))


def score(query, keys):
    return lax.dot_general(query, keys, (((1,), (1,)), ((), ())), preferred_element_type=jnp.float32)


def weigh(probs, values):
    return jnp.dot(probs, values, preferred_element_type=jnp.float32)


def fused_kernel(
    devices,
    q_ref,
    kf_ref,
    vf_ref,
    ks_ref,
    vs_ref,
    tk_ref,
    tv_ref,
    w_ref,
    g_ref,
    t_ref,
    out_ref,
    rows_in,
    text_in,
    gate_in,
    weights,
    weight,
    send,
    near,
    away,
    text,
    piece,
    pieces,
    product,
    load_sem,
    seen,
    near_send,
    near_recv,
    away_send,
    away_recv,
    weight_send,
    weight_recv,
    piece_send,
    piece_across,
    piece_forward,
    piece_far,
    piece_recv,
    back_send,
    back_recv,
):
    groups = lax.axis_index("groups")
    me = lax.axis_index("patch")
    chips = devices // CORES
    group_count = chips
    rows = q_ref.shape[0]
    block_rows = group_count * rows
    text_rows = tk_ref.shape[0]
    part_columns = w_ref.shape[0]
    columns = CORES * part_columns
    chip, core = me // CORES, me % CORES
    block, position = me // group_count, me % group_count
    partner = me + 1 - 2 * core
    side, place = chip % 2, chip // 2
    places = chips // 2
    odd_tile = group_count + position // 2

    def device(index):
        return (groups, index)

    def remote(src, dst, send, recv, index):
        return pltpu.make_async_remote_copy(
            src_ref=src,
            dst_ref=dst,
            send_sem=send,
            recv_sem=recv,
            device_id=device(index),
            device_id_type=MESH,
        )

    def weight_rows(of_core):
        start = pl.multiple_of(of_core * part_columns, part_columns)
        return weights.at[pl.ds(start, part_columns), :]

    loads = [
        pltpu.make_async_copy(ref, rows_in.at[i], load_sem.at[i])
        for i, ref in enumerate((q_ref, kf_ref, vf_ref, ks_ref, vs_ref))
    ]
    for load in loads:
        load.start()

    barrier = pltpu.get_barrier_semaphore()
    has_below, has_above = place > 0, place < places - 1

    def greet(index):
        pl.semaphore_signal(barrier, inc=1, device_id=device(index), device_id_type=MESH)

    @pl.when(has_above)
    def _():
        greet(me + LINES)

    @pl.when(has_below)
    def _():
        greet(me - LINES)

    for step in range(1, LINES):
        greet(place * LINES + (me + step) % LINES)

    full_lanes = pl.ds(pl.multiple_of(position * LANES, LANES), LANES)
    odd_lanes = pl.ds(pl.multiple_of(odd_tile * LANES, LANES), LANES)
    for i, (ref, lanes) in enumerate(
        ((tk_ref, full_lanes), (tv_ref, full_lanes), (tk_ref, odd_lanes), (tv_ref, odd_lanes))
    ):
        loads.append(pltpu.make_async_copy(ref.at[:, lanes], text_in.at[i], load_sem.at[5 + i]))
    chip_columns = pl.ds(pl.multiple_of(chip * columns, LANES), columns)
    loads.append(pltpu.make_async_copy(g_ref.at[:, chip_columns], gate_in, load_sem.at[9]))
    loads.append(pltpu.make_async_copy(w_ref, weight_rows(core), load_sem.at[10]))
    for load in loads[5:]:
        load.start()

    pl.semaphore_wait(
        barrier, LINES - 1 + has_below.astype(jnp.int32) + has_above.astype(jnp.int32)
    )

    def tell(index, about):
        pl.semaphore_signal(seen.at[about], inc=1, device_id=device(index), device_id_type=MESH)

    @pl.when(has_above)
    def _():
        tell(me + LINES, place)

    @pl.when(has_below)
    def _():
        tell(me - LINES, place)

    def hear(other):
        pl.semaphore_wait(seen.at[other], 1)

        @pl.when((other < place) & has_above)
        def _():
            tell(me + LINES, other)

        @pl.when((other > place) & has_below)
        def _():
            tell(me - LINES, other)

    @pl.when(has_below & has_above)
    def _():
        @pl.loop(0, place)
        def _(step):
            hear(place - 1 - step)

        @pl.when(block == 1)
        def _():
            @pl.loop(place + 1, places)
            def _(other):
                hear(other)

    for load in loads[:5]:
        load.wait()
    for g in range(group_count):
        own = slice(g * LANES, (g + 1) * LANES)
        tile = group_count + g // 2
        odd = slice(tile * LANES, (tile + 1) * LANES)
        upper = g % 2 == 1
        half_rows = rows // 2
        sent = (
            rows_in[3, :, own],
            rows_in[4, :, own],
            odd_pair(rows_in[3, :, odd], rows_in[4, :, odd], upper),
            rows_in[0, :, own],
            rows_in[1, :, own],
            rows_in[2, :, own],
            odd_pair(rows_in[1, :, odd], rows_in[2, :, odd], upper),
            odd_pair(rows_in[0, :half_rows, odd], rows_in[0, half_rows:, odd], upper),
        )
        for i, tile_rows in enumerate(sent):
            send[g, i * rows : i * rows + tile_rows.shape[0]] = tile_rows

    def near_copy(target, source):
        return remote(
            send.at[target],
            near.at[source],
            near_send.at[target],
            near_recv.at[source],
            block * group_count + target,
        )

    def away_copy(target, source):
        return remote(
            send.at[target, pl.ds(0, 3 * rows)],
            away.at[source],
            away_send.at[target],
            away_recv.at[source],
            (1 - block) * group_count + target,
        )

    def send_plane(other):
        @pl.loop(0, LINES)
        def _(step):
            target = other % 2 * LINES + (me + step) % LINES

            @pl.when(other // 2 == block)
            def _():
                near_copy(target, position).start()

            @pl.when(other // 2 != block)
            def _():
                away_copy(target, position).start()

    def send_here():
        @pl.loop(1, LINES)
        def _(step):
            near_copy(place % 2 * LINES + (me + step) % LINES, position).start()

    @pl.when(block == 0)
    def _():
        send_here()

        @pl.when(has_below)
        def _():
            send_plane(place - 1)

        @pl.loop(place + 1, places)
        def _(other):
            hear(other)
            send_plane(other)

    @pl.when(block == 1)
    def _():
        @pl.when(jnp.logical_not(has_above))
        def _():
            @pl.loop(0, place)
            def _(step):
                hear(place - 1 - step)

        @pl.when(has_above)
        def _():
            send_plane(2 * block + 1 - place % 2)
            send_plane(1)
            send_plane(0)
            send_here()

        @pl.when(jnp.logical_not(has_above))
        def _():
            send_plane(0)
            send_plane(1)
            send_plane(2 * block + 1 - place % 2)
            send_here()

    pltpu.make_async_copy(send.at[position], near.at[position], near_recv.at[position]).start()
    weight_copy = remote(w_ref, weight_rows(core), weight_send, weight_recv, partner)
    weight_copy.start()

    for load in loads[5:9]:
        load.wait()
    text[...] = jnp.zeros_like(text)
    text[0, :text_rows] = text_in[0]
    text[1, :text_rows] = text_in[1]
    text[2, :text_rows] = jnp.where(
        position % 2 == 1,
        odd_pair(text_in[2], text_in[3], True),
        odd_pair(text_in[2], text_in[3], False),
    )
    loads[9].wait()
    loads[10].wait()
    remote(w_ref, weight_rows(1 - core), weight_send, weight_recv, partner).wait_recv()
    depth = w_ref.shape[1]
    chunk = 2 * LANES

    @pl.loop(0, depth // chunk)
    def _(step):
        at = pl.ds(pl.multiple_of(step * chunk, chunk), chunk)
        weight[at, :] = weights[:, at].T

    scaling = HEAD_DIM**-0.5
    half = block_rows // HALVES
    part_rows = block_rows // PARTS
    odd_rows = part_rows // 2
    padded = text.shape[1]

    def same_patch(stacked):
        query = lax.broadcasted_iota(jnp.int32, (stacked * half, 1), 0) % half // rows
        key = lax.broadcasted_iota(jnp.int32, (1, half), 1) // rows
        return query == key

    def lane_sums(expo):
        sums = expo[:, :LANES]
        for first in range(LANES, expo.shape[1], LANES):
            sums = sums + expo[:, first : first + LANES]
        return sums

    def finish(state, scores, values):
        highest, sums, weighted = state
        peak = jnp.maximum(highest, jnp.max(scores, -1, keepdims=True))
        fade = jnp.exp(highest - peak)
        expo = jnp.exp(scores - peak)
        total = jnp.sum(sums * fade + lane_sums(expo), -1, keepdims=True)
        weighted = weighted * fade + weigh(expo.astype(jnp.bfloat16), values)
        return weighted / total

    @pl.loop(0, group_count)
    def _(source):
        near_copy(position, source).wait_recv()

    def tiles_of(ref, index, first=0, last=group_count):
        at = slice(index * rows, (index + 1) * rows)
        return jnp.concatenate([ref[source, at] for source in range(first, last)], 0)

    low = low_lanes(half)
    half_low = low_lanes(rows // 2)
    per_half = group_count // HALVES
    units = []
    for part in range(HALVES):
        mine = (part * per_half, (part + 1) * per_half)
        pair_query = tiles_of(near, 3, *mine) * jnp.asarray(scaling, near.dtype)
        nothing = jnp.zeros_like(pair_query)
        both = jnp.concatenate(
            [jnp.where(low, pair_query, nothing), jnp.where(low, nothing, pair_query)], 0
        )
        odd_query = []
        for source in range(*mine):
            packed = near[source, 7 * rows :]
            for each in (packed, swap_halves(packed)):
                odd_query.append(jnp.where(half_low, each, jnp.zeros_like(each)))
        odd_query = jnp.concatenate(odd_query, 0) * jnp.asarray(scaling, near.dtype)
        units.append((part, 2, (4, 5, 0, 1), text[0], text[1], both))
        units.append((part, 1, (6, 6, 2, 2), text[2], text[2], odd_query))

    states = []
    last = padded - LANES
    absent = lax.broadcasted_iota(jnp.int32, (1, LANES), 1) >= text_rows - last
    for part, stacked, kinds, text_key, text_value, query in units:
        mine = (part * per_half, (part + 1) * per_half)
        new_key, new_value, old_key, old_value = (tiles_of(near, kind, *mine) for kind in kinds)
        scores = score(query, jnp.concatenate([text_key, old_key, new_key], 0))
        same = same_patch(stacked)
        mixed = jnp.where(same, scores[:, padded + half :], scores[:, padded : padded + half])
        scores = jnp.concatenate(
            [scores[:, :last], jnp.where(absent, NEVER, scores[:, last:padded]), mixed], 1
        )
        peak = jnp.max(scores, -1, keepdims=True)
        expo = jnp.exp(scores - peak)
        mixed = expo[:, padded:]
        probs = [expo[:, :padded], jnp.where(same, 0.0, mixed), jnp.where(same, mixed, 0.0)]
        probs = jnp.concatenate([each.astype(jnp.bfloat16) for each in probs], 1)
        values = jnp.concatenate([text_value, old_value, new_value], 0)
        states.append((peak, lane_sums(expo), weigh(probs, values)))

    @pl.loop(0, group_count)
    def _(source):
        away_copy(position, source).wait_recv()

    def column_copy(part, target_place, source):
        return remote(
            piece.at[part],
            pieces.at[part, source],
            piece_send.at[part, target_place],
            piece_recv.at[part, source],
            (target_place * 2 + side) * CORES + block,
        )

    def across_copy(part):
        return remote(
            piece.at[part],
            pieces.at[part, position],
            piece_across.at[part],
            piece_recv.at[part, position],
            (place * 2 + 1 - side) * CORES + block,
        )

    def forward_copy(part, source, index):
        return remote(
            pieces.at[part, source],
            pieces.at[part, source],
            piece_forward.at[part, index],
            piece_recv.at[part, source],
            (place * 2 + 1 - side) * CORES + core,
        )

    def far_copy(part, source, index):
        return remote(
            pieces.at[part, source],
            pieces.at[part, source],
            piece_far.at[part, index],
            piece_recv.at[part, source],
            ((1 - core) * (places - 1) * 2 + side) * CORES + core,
        )

    mate = 2 * block + 1 - place % 2
    gate = 2 - block
    at_gate = place == 2 - core
    elsewhere = place // 2 != core

    part_low = low_lanes(part_rows)
    odd_low = low_lanes(odd_rows)
    done = []
    for part in range(PARTS):
        if part % (PARTS // HALVES) == 0:
            done = []
            first_unit = 2 * (part * HALVES // PARTS)
            for i in (first_unit, first_unit + 1):
                _, _, kinds, _, _, query = units[i]
                key, value = (tiles_of(away, kind) for kind in kinds[2:])
                done.append(finish(states[i], score(query, key), value))
        at = part % (PARTS // HALVES) * part_rows
        piece[part, :part_rows] = jnp.where(
            part_low, done[0][at : at + part_rows], done[0][half + at : half + at + part_rows]
        ).astype(piece.dtype)
        piece[part, part_rows:] = jnp.where(
            odd_low,
            pltpu.roll(done[1][at : at + odd_rows], HEAD_DIM, 1),
            done[1][at + odd_rows : at + part_rows],
        ).astype(piece.dtype)

        column_copy(part, gate, position).start()
        column_copy(part, mate, position).start()
        across_copy(part).start()

    for part in range(PARTS):

        @pl.when(core == block)
        def _():
            pltpu.make_async_copy(
                piece.at[part], pieces.at[part, position], piece_recv.at[part, position]
            ).start()

        @pl.when(core != block)
        def _():
            column_copy(part, place, position).start()

    def column_source(index, of_side):
        return index // CORES * 2 * CORES + of_side * CORES + index % CORES

    column_pieces = group_count // 2

    for part in range(PARTS):

        @pl.loop(0, column_pieces)
        def _(index):
            index = (index + (1 - core) * CORES) % column_pieces
            source = column_source(index, side)
            column_copy(part, place, source).wait_recv()

            @pl.when(at_gate)
            def _():
                far_copy(part, source, index).start()

            @pl.when(elsewhere | (index // CORES != place % 2))
            def _():
                forward_copy(part, source, index).start()

    def back_copy(target, source):
        return remote(
            product.at[target],
            out_ref.at[:, pl.ds(pl.multiple_of(source * columns, LANES), columns)],
            back_send.at[target],
            back_recv.at[source],
            core * group_count + target,
        )

    gating = gate_in[pl.ds(t_ref[0], 1), :]
    patches = group_count // PARTS
    for part in range(PARTS):

        @pl.loop(0, column_pieces)
        def _(index):
            column_copy(part, place, column_source(index, 1 - side)).wait_recv()

        tiles = [pieces[part, g, :part_rows] for g in range(group_count)]
        for pair in range(group_count // 2):
            even = pieces[part, 2 * pair, part_rows:]
            upper = pieces[part, 2 * pair + 1, part_rows:]
            top = jnp.where(odd_low, even, swap_halves(upper))
            bottom = jnp.where(odd_low, swap_halves(even), upper)
            tiles.append(jnp.concatenate([top, bottom], 0))
        attended = jnp.concatenate(tiles, 1)
        projected = jnp.dot(attended, weight[...], preferred_element_type=jnp.float32)
        product[part * patches : (part + 1) * patches] = (
            (projected * gating).astype(product.dtype).reshape(patches, rows, columns)
        )

        @pl.loop(0, patches)
        def _(step):
            target = part * patches + (position + step) % patches

            @pl.when(core * group_count + target != me)
            def _():
                back_copy(target, chip).start()

        @pl.when((core == block) & (position // patches == part))
        def _():
            pltpu.make_async_copy(
                product.at[position],
                out_ref.at[:, chip_columns],
                back_recv.at[chip],
            ).start()

    @pl.loop(1, group_count)
    def _(step):
        near_copy((position + step) % group_count, position).wait_send()

    @pl.loop(0, group_count)
    def _(target):
        away_copy(target, position).wait_send()

    weight_copy.wait_send()

    for part in range(PARTS):

        column_copy(part, gate, position).wait_send()
        across_copy(part).wait_send()
        column_copy(part, mate, position).wait_send()

        @pl.when(core != block)
        def _():
            column_copy(part, place, position).wait_send()

        @pl.loop(0, column_pieces)
        def _(index):
            source = column_source(index, side)

            @pl.when(at_gate)
            def _():
                far_copy(part, source, index).wait_send()

            @pl.when(elsewhere | (index // CORES != place % 2))
            def _():
                forward_copy(part, source, index).wait_send()

    @pl.loop(0, group_count)
    def _(target):
        @pl.when(core * group_count + target != me)
        def _():
            back_copy(target, chip).wait_send()

    @pl.loop(0, chips)
    def _(source):
        back_copy(position, source).wait_recv()


def fused_body(
    queries,
    fresh_keys,
    fresh_values,
    stale_keys,
    stale_values,
    text_keys,
    text_values,
    out_weight,
    gate_table,
    timestep,
):
    devices = lax.axis_size("patch")
    chips = devices // CORES
    group_count = chips
    rows, width = queries.shape
    block_rows = group_count * rows
    piece_rows = (block_rows + block_rows // 2) // PARTS
    text_rows = text_keys.shape[0]
    padded = -(-text_rows // LANES) * LANES
    depth, part_columns = out_weight.shape
    columns = CORES * part_columns
    bf16 = jnp.bfloat16
    dma = pltpu.SemaphoreType.DMA
    anywhere = pl.BlockSpec(memory_space=pl.ANY)
    return pl.pallas_call(
        functools.partial(fused_kernel, devices),
        out_shape=pltpu.VMEM((rows, part_columns * devices), bf16),
        in_specs=[anywhere] * 9 + [pl.BlockSpec(memory_space=pltpu.SMEM)],
        out_specs=pl.BlockSpec(memory_space=pltpu.VMEM),
        scratch_shapes=[
            pltpu.VMEM((5, rows, width), bf16),
            pltpu.VMEM((4, text_rows, LANES), bf16),
            pltpu.VMEM((gate_table.shape[0], columns), jnp.float32),
            pltpu.VMEM((columns, depth), bf16),
            pltpu.VMEM((depth, columns), bf16),
            pltpu.VMEM((group_count, 7 * rows + rows // 2, LANES), bf16),
            pltpu.VMEM((group_count, 7 * rows + rows // 2, LANES), bf16),
            pltpu.VMEM((group_count, 3 * rows, LANES), bf16),
            pltpu.VMEM((3, padded, LANES), bf16),
            pltpu.VMEM((PARTS, piece_rows, LANES), bf16),
            pltpu.VMEM((PARTS, group_count, piece_rows, LANES), bf16),
            pltpu.VMEM((group_count, rows, columns), bf16),
            dma((11,)),
            pltpu.SemaphoreType.REGULAR((chips // 2,)),
            dma((group_count,)),
            dma((group_count,)),
            dma((group_count,)),
            dma((group_count,)),
            dma,
            dma,
            dma((PARTS, chips // 2)),
            dma((PARTS,)),
            dma((PARTS, group_count // 2)),
            dma((PARTS, group_count // 2)),
            dma((PARTS, group_count)),
            dma((group_count,)),
            dma((chips,)),
        ],
        compiler_params=pltpu.CompilerParams(collective_id=0, has_side_effects=True),
    )(
        queries,
        fresh_keys,
        fresh_values,
        stale_keys,
        stale_values,
        text_keys,
        text_values,
        out_weight.T,
        gate_table,
        timestep,
    )


def solution(mesh):
    in_specs = (
        P(("groups", "patch"), None),
        P(("groups", "patch"), None),
        P(("groups", "patch"), None),
        P(("groups", "patch"), None),
        P(("groups", "patch"), None),
        P("groups", None),
        P("groups", None),
        P(None, "patch"),
        P(),
        P("groups"),
    )
    out_specs = P(("groups", "patch"), None)
    chosen = fused_body if fused_fits(mesh) else body
    return jax.shard_map(chosen, mesh=mesh, in_specs=in_specs, out_specs=out_specs, check_vma=False)
```

```python
import functools
import math

import jax
import jax.numpy as jnp
from jax import lax
from jax.experimental import pallas as pl
from jax.experimental.pallas import tpu as pltpu
from jax.sharding import PartitionSpec as P

HEAD_DIM = 64
HEADS = 24


def from_behind(shard, axis, by):
    peers = lax.axis_size(axis)
    return lax.ppermute(shard, axis, [(i, (i + by) % peers) for i in range(peers)])


def pick_group(stacked, position):
    return lax.dynamic_index_in_dim(stacked, position, 0, keepdims=False)


def by_group(matrix, group_count):
    width = matrix.shape[1] // group_count
    return matrix.reshape(matrix.shape[0], group_count, width).transpose(1, 0, 2)


def gather_block(stacked, group_count, position):
    received = [pick_group(stacked, position)]
    for step_size in range(1, group_count):
        payload = pick_group(stacked, (position + step_size) % group_count)
        arrived = []
        for offset_by in (step_size, step_size - group_count):
            arrived.append(from_behind(payload, "patch", offset_by))
        received.append(jnp.where(position >= step_size, arrived[0], arrived[1]))
    ordered = jnp.stack(received, 0)
    order = (position - jnp.arange(group_count, dtype=jnp.int32)) % group_count
    return jnp.take(ordered, order, axis=0)


def return_block(stacked, group_count, position):
    received = [pick_group(stacked, position)]
    for step_size in range(1, group_count):
        payload = pick_group(stacked, (position + step_size) % group_count)
        arrived = []
        for offset_by in (step_size, step_size - group_count):
            arrived.append(from_behind(payload, "patch", offset_by))
        received.append(jnp.where(position >= step_size, arrived[0], arrived[1]))
    ordered = jnp.stack(received, 0)
    order = (position - jnp.arange(group_count, dtype=jnp.int32)) % group_count
    return jnp.take(ordered, order, axis=0)


def body(
    queries,
    fresh_keys,
    fresh_values,
    stale_keys,
    stale_values,
    text_keys,
    text_values,
    out_weight,
    gate_table,
    timestep,
):
    row_count = queries.shape[0]
    head_count = HEADS
    head_width = HEAD_DIM
    scaling = head_width ** (-0.5)
    group_count = math.gcd(head_count, 8)
    group_heads = head_count // group_count
    group_width = group_heads * head_width
    device_count = lax.axis_size("patch")
    position = lax.axis_index("patch") % group_count
    block_first = lax.axis_index("patch") // group_count * group_count
    local_stack = jnp.stack(
        [
            by_group(queries, group_count),
            by_group(fresh_keys, group_count),
            by_group(fresh_values, group_count),
        ],
        1,
    )
    block_stack = gather_block(local_stack, group_count, position)
    block_rows_count = group_count * row_count
    block_query = block_stack[:, 0].reshape(block_rows_count, group_heads, head_width)
    block_keys = block_stack[:, 1].reshape(block_rows_count, group_heads, head_width)
    block_values = block_stack[:, 2].reshape(block_rows_count, group_heads, head_width)
    spread_keys = jnp.tile(by_group(stale_keys, group_count), (device_count // group_count, 1, 1))
    spread_values = jnp.tile(
        by_group(stale_values, group_count), (device_count // group_count, 1, 1)
    )
    every_keys, every_values = (
        lax.all_to_all(spread_keys, "patch", split_axis=0, concat_axis=0, tiled=True),
        lax.all_to_all(spread_values, "patch", split_axis=0, concat_axis=0, tiled=True),
    )
    every_keys = every_keys.reshape(device_count * row_count, group_heads, head_width)
    every_values = every_values.reshape(device_count * row_count, group_heads, head_width)
    text_k = pick_group(by_group(text_keys, group_count), position).reshape(
        -1, group_heads, head_width
    )
    text_v = pick_group(by_group(text_values, group_count), position).reshape(
        -1, group_heads, head_width
    )
    query_patch = jnp.arange(block_rows_count, dtype=jnp.int32) // row_count
    stale_patch = jnp.arange(device_count * row_count, dtype=jnp.int32) // row_count
    stale_mask = stale_patch[None, :] != (block_first + query_patch)[:, None]
    fresh_mask = query_patch[None, :] == query_patch[:, None]

    def scored(key_block):
        return (
            jnp.einsum("qhd,khd->qhk", block_query, key_block, preferred_element_type=jnp.float32)
            * scaling
        )

    text_scores = scored(text_k)
    fresh_scores = jnp.where(fresh_mask[:, None, :], scored(block_keys), -1e30)
    stale_scores = jnp.where(stale_mask[:, None, :], scored(every_keys), -1e30)
    highest = jnp.maximum(
        jnp.maximum(jnp.max(text_scores, -1), jnp.max(fresh_scores, -1)), jnp.max(stale_scores, -1)
    )
    text_expo = jnp.exp(text_scores - highest[..., None])
    fresh_expo = jnp.exp(fresh_scores - highest[..., None])
    stale_expo = jnp.exp(stale_scores - highest[..., None])
    total = jnp.sum(text_expo, -1) + jnp.sum(fresh_expo, -1) + jnp.sum(stale_expo, -1)

    def weigh_block(expo, value_block):
        return jnp.einsum(
            "qhk,khd->qhd",
            expo.astype(jnp.bfloat16),
            value_block,
            preferred_element_type=jnp.float32,
        )

    weighted = (
        weigh_block(text_expo, text_v)
        + weigh_block(fresh_expo, block_values)
        + weigh_block(stale_expo, every_values)
    )
    block_out = (
        (weighted / total[..., None])
        .reshape(group_count, row_count, group_width)
        .astype(jnp.bfloat16)
    )
    home = return_block(block_out, group_count, position)
    attended = home.transpose(1, 0, 2).reshape(row_count, head_count * head_width)
    projected = jnp.dot(
        attended,
        lax.all_gather(out_weight, "patch", axis=1, tiled=True),
        preferred_element_type=jnp.float32,
    )
    selector = (jnp.arange(gate_table.shape[0], dtype=jnp.int32) == timestep[0]).astype(jnp.float32)
    gating = jnp.dot(selector, gate_table, precision=lax.Precision.HIGHEST)
    return (projected * gating[None, :]).astype(jnp.bfloat16)


LANES = 128
CORES = 2
LINES = 4
HALVES = 1
PARTS = 4
NEVER = -1e30
MESH = pl.DeviceIdType.MESH


def fused_fits(mesh):
    chips = mesh.shape["patch"] // CORES
    return (
        2 * HEAD_DIM == LANES
        and mesh.shape["patch"] % (2 * CORES) == 0
        and HEADS == 3 * chips
        and chips == math.gcd(HEADS, 8)
        and chips == 4 * CORES
    )


def swap_halves(tile):
    return pltpu.roll(tile.astype(jnp.float32), HEAD_DIM, 1).astype(tile.dtype)


def low_lanes(rows):
    return lax.broadcasted_iota(jnp.int32, (rows, LANES), 1) < HEAD_DIM


def odd_pair(first, second, upper):
    low = low_lanes(first.shape[0])
    if upper:
        return jnp.where(low, swap_halves(first), second)
    return jnp.where(low, first, swap_halves(second))


def score(query, keys):
    return lax.dot_general(query, keys, (((1,), (1,)), ((), ())), preferred_element_type=jnp.float32)


def weigh(probs, values):
    return jnp.dot(probs, values, preferred_element_type=jnp.float32)


def fused_kernel(
    devices,
    q_ref,
    kf_ref,
    vf_ref,
    ks_ref,
    vs_ref,
    tk_ref,
    tv_ref,
    w_ref,
    g_ref,
    t_ref,
    out_ref,
    rows_in,
    text_in,
    gate_in,
    weights,
    weight,
    send,
    near,
    away,
    text,
    piece,
    pieces,
    product,
    load_sem,
    seen,
    near_send,
    near_recv,
    away_send,
    away_recv,
    weight_send,
    weight_recv,
    piece_send,
    piece_across,
    piece_forward,
    piece_far,
    piece_recv,
    back_send,
    back_recv,
):
    groups = lax.axis_index("groups")
    me = lax.axis_index("patch")
    chips = devices // CORES
    group_count = chips
    rows = q_ref.shape[0]
    block_rows = group_count * rows
    text_rows = tk_ref.shape[0]
    part_columns = w_ref.shape[0]
    columns = CORES * part_columns
    chip, core = me // CORES, me % CORES
    block, position = me // group_count, me % group_count
    partner = me + 1 - 2 * core
    side, place = chip % 2, chip // 2
    places = chips // 2
    odd_tile = group_count + position // 2

    def device(index):
        return (groups, index)

    def remote(src, dst, send, recv, index):
        return pltpu.make_async_remote_copy(
            src_ref=src,
            dst_ref=dst,
            send_sem=send,
            recv_sem=recv,
            device_id=device(index),
            device_id_type=MESH,
        )

    def weight_rows(of_core):
        start = pl.multiple_of(of_core * part_columns, part_columns)
        return weights.at[pl.ds(start, part_columns), :]

    loads = [
        pltpu.make_async_copy(ref, rows_in.at[i], load_sem.at[i])
        for i, ref in enumerate((q_ref, kf_ref, vf_ref, ks_ref, vs_ref))
    ]
    for load in loads:
        load.start()

    barrier = pltpu.get_barrier_semaphore()
    has_below, has_above = place > 0, place < places - 1

    def greet(index):
        pl.semaphore_signal(barrier, inc=1, device_id=device(index), device_id_type=MESH)

    @pl.when(has_above)
    def _():
        greet(me + LINES)

    @pl.when(has_below)
    def _():
        greet(me - LINES)

    for step in range(1, LINES):
        greet(place * LINES + (me + step) % LINES)

    full_lanes = pl.ds(pl.multiple_of(position * LANES, LANES), LANES)
    odd_lanes = pl.ds(pl.multiple_of(odd_tile * LANES, LANES), LANES)
    for i, (ref, lanes) in enumerate(
        ((tk_ref, full_lanes), (tv_ref, full_lanes), (tk_ref, odd_lanes), (tv_ref, odd_lanes))
    ):
        loads.append(pltpu.make_async_copy(ref.at[:, lanes], text_in.at[i], load_sem.at[5 + i]))
    chip_columns = pl.ds(pl.multiple_of(chip * columns, LANES), columns)
    loads.append(pltpu.make_async_copy(g_ref.at[:, chip_columns], gate_in, load_sem.at[9]))
    loads.append(pltpu.make_async_copy(w_ref, weight_rows(core), load_sem.at[10]))
    for load in loads[5:]:
        load.start()

    pl.semaphore_wait(
        barrier, LINES - 1 + has_below.astype(jnp.int32) + has_above.astype(jnp.int32)
    )

    def tell(index, about):
        pl.semaphore_signal(seen.at[about], inc=1, device_id=device(index), device_id_type=MESH)

    @pl.when(has_above)
    def _():
        tell(me + LINES, place)

    @pl.when(has_below)
    def _():
        tell(me - LINES, place)

    def hear(other):
        pl.semaphore_wait(seen.at[other], 1)

        @pl.when((other < place) & has_above)
        def _():
            tell(me + LINES, other)

        @pl.when((other > place) & has_below)
        def _():
            tell(me - LINES, other)

    @pl.when(has_below & has_above)
    def _():
        @pl.loop(0, place)
        def _(step):
            hear(place - 1 - step)

        @pl.when(block == 1)
        def _():
            @pl.loop(place + 1, places)
            def _(other):
                hear(other)

    for load in loads[:5]:
        load.wait()
    for g in range(group_count):
        own = slice(g * LANES, (g + 1) * LANES)
        tile = group_count + g // 2
        odd = slice(tile * LANES, (tile + 1) * LANES)
        upper = g % 2 == 1
        half_rows = rows // 2
        sent = (
            rows_in[3, :, own],
            rows_in[4, :, own],
            odd_pair(rows_in[3, :, odd], rows_in[4, :, odd], upper),
            rows_in[0, :, own],
            rows_in[1, :, own],
            rows_in[2, :, own],
            odd_pair(rows_in[1, :, odd], rows_in[2, :, odd], upper),
            odd_pair(rows_in[0, :half_rows, odd], rows_in[0, half_rows:, odd], upper),
        )
        for i, tile_rows in enumerate(sent):
            send[g, i * rows : i * rows + tile_rows.shape[0]] = tile_rows

    def near_copy(target, source):
        return remote(
            send.at[target],
            near.at[source],
            near_send.at[target],
            near_recv.at[source],
            block * group_count + target,
        )

    def away_copy(target, source):
        return remote(
            send.at[target, pl.ds(0, 3 * rows)],
            away.at[source],
            away_send.at[target],
            away_recv.at[source],
            (1 - block) * group_count + target,
        )

    def send_plane(other):
        @pl.loop(0, LINES)
        def _(step):
            target = other % 2 * LINES + (me + step) % LINES

            @pl.when(other // 2 == block)
            def _():
                near_copy(target, position).start()

            @pl.when(other // 2 != block)
            def _():
                away_copy(target, position).start()

    def send_here():
        @pl.loop(1, LINES)
        def _(step):
            near_copy(place % 2 * LINES + (me + step) % LINES, position).start()

    @pl.when(block == 0)
    def _():
        @pl.when(has_below)
        def _():
            send_plane(place - 1)
            send_here()

        @pl.loop(place + 1, places)
        def _(other):
            hear(other)
            send_plane(other)

            @pl.when(jnp.logical_not(has_below) & (other == place + 1))
            def _():
                send_here()

    @pl.when(block == 1)
    def _():
        @pl.when(jnp.logical_not(has_above))
        def _():
            @pl.loop(0, place)
            def _(step):
                hear(place - 1 - step)

        @pl.when(has_above)
        def _():
            send_plane(2 * block + 1 - place % 2)
            send_plane(1)
            send_plane(0)
            send_here()

        @pl.when(jnp.logical_not(has_above))
        def _():
            send_plane(0)
            send_plane(1)
            send_plane(2 * block + 1 - place % 2)
            send_here()

    pltpu.make_async_copy(send.at[position], near.at[position], near_recv.at[position]).start()
    weight_copy = remote(w_ref, weight_rows(core), weight_send, weight_recv, partner)
    weight_copy.start()

    for load in loads[5:9]:
        load.wait()
    text[...] = jnp.zeros_like(text)
    text[0, :text_rows] = text_in[0]
    text[1, :text_rows] = text_in[1]
    text[2, :text_rows] = jnp.where(
        position % 2 == 1,
        odd_pair(text_in[2], text_in[3], True),
        odd_pair(text_in[2], text_in[3], False),
    )
    loads[9].wait()
    loads[10].wait()
    remote(w_ref, weight_rows(1 - core), weight_send, weight_recv, partner).wait_recv()
    depth = w_ref.shape[1]
    chunk = 2 * LANES

    @pl.loop(0, depth // chunk)
    def _(step):
        at = pl.ds(pl.multiple_of(step * chunk, chunk), chunk)
        weight[at, :] = weights[:, at].T

    scaling = HEAD_DIM**-0.5
    half = block_rows // HALVES
    part_rows = block_rows // PARTS
    odd_rows = part_rows // 2
    padded = text.shape[1]

    def same_patch(stacked):
        query = lax.broadcasted_iota(jnp.int32, (stacked * half, 1), 0) % half // rows
        key = lax.broadcasted_iota(jnp.int32, (1, half), 1) // rows
        return query == key

    def lane_sums(expo):
        sums = expo[:, :LANES]
        for first in range(LANES, expo.shape[1], LANES):
            sums = sums + expo[:, first : first + LANES]
        return sums

    def finish(state, scores, values):
        highest, sums, weighted = state
        peak = jnp.maximum(highest, jnp.max(scores, -1, keepdims=True))
        fade = jnp.exp(highest - peak)
        expo = jnp.exp(scores - peak)
        total = jnp.sum(sums * fade + lane_sums(expo), -1, keepdims=True)
        weighted = weighted * fade + weigh(expo.astype(jnp.bfloat16), values)
        return weighted / total

    @pl.loop(0, group_count)
    def _(source):
        near_copy(position, source).wait_recv()

    def tiles_of(ref, index, first=0, last=group_count):
        at = slice(index * rows, (index + 1) * rows)
        return jnp.concatenate([ref[source, at] for source in range(first, last)], 0)

    low = low_lanes(half)
    half_low = low_lanes(rows // 2)
    per_half = group_count // HALVES
    units = []
    for part in range(HALVES):
        mine = (part * per_half, (part + 1) * per_half)
        pair_query = tiles_of(near, 3, *mine) * jnp.asarray(scaling, near.dtype)
        nothing = jnp.zeros_like(pair_query)
        both = jnp.concatenate(
            [jnp.where(low, pair_query, nothing), jnp.where(low, nothing, pair_query)], 0
        )
        odd_query = []
        for source in range(*mine):
            packed = near[source, 7 * rows :]
            for each in (packed, swap_halves(packed)):
                odd_query.append(jnp.where(half_low, each, jnp.zeros_like(each)))
        odd_query = jnp.concatenate(odd_query, 0) * jnp.asarray(scaling, near.dtype)
        units.append((part, 2, (4, 5, 0, 1), text[0], text[1], both))
        units.append((part, 1, (6, 6, 2, 2), text[2], text[2], odd_query))

    states = []
    last = padded - LANES
    absent = lax.broadcasted_iota(jnp.int32, (1, LANES), 1) >= text_rows - last
    for part, stacked, kinds, text_key, text_value, query in units:
        mine = (part * per_half, (part + 1) * per_half)
        new_key, new_value, old_key, old_value = (tiles_of(near, kind, *mine) for kind in kinds)
        scores = score(query, jnp.concatenate([text_key, old_key, new_key], 0))
        same = same_patch(stacked)
        mixed = jnp.where(same, scores[:, padded + half :], scores[:, padded : padded + half])
        scores = jnp.concatenate(
            [scores[:, :last], jnp.where(absent, NEVER, scores[:, last:padded]), mixed], 1
        )
        peak = jnp.max(scores, -1, keepdims=True)
        expo = jnp.exp(scores - peak)
        mixed = expo[:, padded:]
        probs = [expo[:, :padded], jnp.where(same, 0.0, mixed), jnp.where(same, mixed, 0.0)]
        probs = jnp.concatenate([each.astype(jnp.bfloat16) for each in probs], 1)
        values = jnp.concatenate([text_value, old_value, new_value], 0)
        states.append((peak, lane_sums(expo), weigh(probs, values)))

    @pl.loop(0, group_count)
    def _(source):
        away_copy(position, source).wait_recv()

    def column_copy(part, target_place, source):
        return remote(
            piece.at[part],
            pieces.at[part, source],
            piece_send.at[part, target_place],
            piece_recv.at[part, source],
            (target_place * 2 + side) * CORES + block,
        )

    def across_copy(part):
        return remote(
            piece.at[part],
            pieces.at[part, position],
            piece_across.at[part],
            piece_recv.at[part, position],
            (place * 2 + 1 - side) * CORES + block,
        )

    def forward_copy(part, source, index):
        return remote(
            pieces.at[part, source],
            pieces.at[part, source],
            piece_forward.at[part, index],
            piece_recv.at[part, source],
            (place * 2 + 1 - side) * CORES + core,
        )

    def far_copy(part, source, index):
        return remote(
            pieces.at[part, source],
            pieces.at[part, source],
            piece_far.at[part, index],
            piece_recv.at[part, source],
            ((1 - core) * (places - 1) * 2 + side) * CORES + core,
        )

    mate = 2 * block + 1 - place % 2
    gate = 2 - block
    at_gate = place == 2 - core
    elsewhere = place // 2 != core

    part_low = low_lanes(part_rows)
    odd_low = low_lanes(odd_rows)
    done = []
    for part in range(PARTS):
        if part % (PARTS // HALVES) == 0:
            done = []
            first_unit = 2 * (part * HALVES // PARTS)
            for i in (first_unit, first_unit + 1):
                _, _, kinds, _, _, query = units[i]
                key, value = (tiles_of(away, kind) for kind in kinds[2:])
                done.append(finish(states[i], score(query, key), value))
        at = part % (PARTS // HALVES) * part_rows
        piece[part, :part_rows] = jnp.where(
            part_low, done[0][at : at + part_rows], done[0][half + at : half + at + part_rows]
        ).astype(piece.dtype)
        piece[part, part_rows:] = jnp.where(
            odd_low,
            pltpu.roll(done[1][at : at + odd_rows], HEAD_DIM, 1),
            done[1][at + odd_rows : at + part_rows],
        ).astype(piece.dtype)

        column_copy(part, gate, position).start()
        column_copy(part, mate, position).start()
        across_copy(part).start()

    for part in range(PARTS):

        @pl.when(core == block)
        def _():
            pltpu.make_async_copy(
                piece.at[part], pieces.at[part, position], piece_recv.at[part, position]
            ).start()

        @pl.when(core != block)
        def _():
            column_copy(part, place, position).start()

    def column_source(index, of_side):
        return index // CORES * 2 * CORES + of_side * CORES + index % CORES

    column_pieces = group_count // 2

    for part in range(PARTS):

        @pl.loop(0, column_pieces)
        def _(index):
            index = (index + (1 - core) * CORES) % column_pieces
            source = column_source(index, side)
            column_copy(part, place, source).wait_recv()

            @pl.when(at_gate)
            def _():
                far_copy(part, source, index).start()

            @pl.when(elsewhere | (index // CORES != place % 2))
            def _():
                forward_copy(part, source, index).start()

    def back_copy(target, source):
        return remote(
            product.at[target],
            out_ref.at[:, pl.ds(pl.multiple_of(source * columns, LANES), columns)],
            back_send.at[target],
            back_recv.at[source],
            core * group_count + target,
        )

    gating = gate_in[pl.ds(t_ref[0], 1), :]
    patches = group_count // PARTS
    for part in range(PARTS):

        @pl.loop(0, column_pieces)
        def _(index):
            column_copy(part, place, column_source(index, 1 - side)).wait_recv()

        tiles = [pieces[part, g, :part_rows] for g in range(group_count)]
        for pair in range(group_count // 2):
            even = pieces[part, 2 * pair, part_rows:]
            upper = pieces[part, 2 * pair + 1, part_rows:]
            top = jnp.where(odd_low, even, swap_halves(upper))
            bottom = jnp.where(odd_low, swap_halves(even), upper)
            tiles.append(jnp.concatenate([top, bottom], 0))
        attended = jnp.concatenate(tiles, 1)
        projected = jnp.dot(attended, weight[...], preferred_element_type=jnp.float32)
        product[part * patches : (part + 1) * patches] = (
            (projected * gating).astype(product.dtype).reshape(patches, rows, columns)
        )

        @pl.loop(0, patches)
        def _(step):
            target = part * patches + (position + step) % patches

            @pl.when(core * group_count + target != me)
            def _():
                back_copy(target, chip).start()

        @pl.when((core == block) & (position // patches == part))
        def _():
            pltpu.make_async_copy(
                product.at[position],
                out_ref.at[:, chip_columns],
                back_recv.at[chip],
            ).start()

    @pl.loop(1, group_count)
    def _(step):
        near_copy((position + step) % group_count, position).wait_send()

    @pl.loop(0, group_count)
    def _(target):
        away_copy(target, position).wait_send()

    weight_copy.wait_send()

    for part in range(PARTS):

        column_copy(part, gate, position).wait_send()
        across_copy(part).wait_send()
        column_copy(part, mate, position).wait_send()

        @pl.when(core != block)
        def _():
            column_copy(part, place, position).wait_send()

        @pl.loop(0, column_pieces)
        def _(index):
            source = column_source(index, side)

            @pl.when(at_gate)
            def _():
                far_copy(part, source, index).wait_send()

            @pl.when(elsewhere | (index // CORES != place % 2))
            def _():
                forward_copy(part, source, index).wait_send()

    @pl.loop(0, group_count)
    def _(target):
        @pl.when(core * group_count + target != me)
        def _():
            back_copy(target, chip).wait_send()

    @pl.loop(0, chips)
    def _(source):
        back_copy(position, source).wait_recv()


def fused_body(
    queries,
    fresh_keys,
    fresh_values,
    stale_keys,
    stale_values,
    text_keys,
    text_values,
    out_weight,
    gate_table,
    timestep,
):
    devices = lax.axis_size("patch")
    chips = devices // CORES
    group_count = chips
    rows, width = queries.shape
    block_rows = group_count * rows
    piece_rows = (block_rows + block_rows // 2) // PARTS
    text_rows = text_keys.shape[0]
    padded = -(-text_rows // LANES) * LANES
    depth, part_columns = out_weight.shape
    columns = CORES * part_columns
    bf16 = jnp.bfloat16
    dma = pltpu.SemaphoreType.DMA
    anywhere = pl.BlockSpec(memory_space=pl.ANY)
    return pl.pallas_call(
        functools.partial(fused_kernel, devices),
        out_shape=pltpu.VMEM((rows, part_columns * devices), bf16),
        in_specs=[anywhere] * 9 + [pl.BlockSpec(memory_space=pltpu.SMEM)],
        out_specs=pl.BlockSpec(memory_space=pltpu.VMEM),
        scratch_shapes=[
            pltpu.VMEM((5, rows, width), bf16),
            pltpu.VMEM((4, text_rows, LANES), bf16),
            pltpu.VMEM((gate_table.shape[0], columns), jnp.float32),
            pltpu.VMEM((columns, depth), bf16),
            pltpu.VMEM((depth, columns), bf16),
            pltpu.VMEM((group_count, 7 * rows + rows // 2, LANES), bf16),
            pltpu.VMEM((group_count, 7 * rows + rows // 2, LANES), bf16),
            pltpu.VMEM((group_count, 3 * rows, LANES), bf16),
            pltpu.VMEM((3, padded, LANES), bf16),
            pltpu.VMEM((PARTS, piece_rows, LANES), bf16),
            pltpu.VMEM((PARTS, group_count, piece_rows, LANES), bf16),
            pltpu.VMEM((group_count, rows, columns), bf16),
            dma((11,)),
            pltpu.SemaphoreType.REGULAR((chips // 2,)),
            dma((group_count,)),
            dma((group_count,)),
            dma((group_count,)),
            dma((group_count,)),
            dma,
            dma,
            dma((PARTS, chips // 2)),
            dma((PARTS,)),
            dma((PARTS, group_count // 2)),
            dma((PARTS, group_count // 2)),
            dma((PARTS, group_count)),
            dma((group_count,)),
            dma((chips,)),
        ],
        compiler_params=pltpu.CompilerParams(collective_id=0, has_side_effects=True),
    )(
        queries,
        fresh_keys,
        fresh_values,
        stale_keys,
        stale_values,
        text_keys,
        text_values,
        out_weight.T,
        gate_table,
        timestep,
    )


def solution(mesh):
    in_specs = (
        P(("groups", "patch"), None),
        P(("groups", "patch"), None),
        P(("groups", "patch"), None),
        P(("groups", "patch"), None),
        P(("groups", "patch"), None),
        P("groups", None),
        P("groups", None),
        P(None, "patch"),
        P(),
        P("groups"),
    )
    out_specs = P(("groups", "patch"), None)
    chosen = fused_body if fused_fits(mesh) else body
    return jax.shard_map(chosen, mesh=mesh, in_specs=in_specs, out_specs=out_specs, check_vma=False)
```
